32 devices in a mesh: data: 4 (over y, z), stage: 8 (over x, core).
Axes of the slice: x: 4, y: 2, z: 2, core: 2. Of those that a mesh axis runs over, the one named last changes fastest.
The devices are a block of a 4x4x8 slice.
Arguments:
- x_init: float32 [4, 256, 16], P('data'), parts along dimension 0
- w_in: bfloat16 [16, 384], replicated
- w_out: bfloat16 [384, 16], replicated
- w_qkv: bfloat16 [8, 384, 1152], P('stage')
- w_proj: bfloat16 [8, 6, 64, 384], P('stage')
- w_up: bfloat16 [8, 384, 1536], P('stage')
- w_down: bfloat16 [8, 1536, 384], P('stage')
- mod_table: float32 [32, 8, 6, 384], P(None, 'stage')
- coef_keep: float32 [32], replicated
- coef_noise: float32 [32], replicated
- h_warm: bfloat16 [2, 7, 4, 256, 384], P(None, None, 'data'), parts along dimension 2
Outputs:
- output: float32 [4, 256, 16], P('data'), parts along dimension 0
There are 4 independent parts. The reference program is written for one: setup_inputs(seed, part) draws one part's arguments, and reference() takes and returns one part's arrays. A program takes and returns all parts, laid end to end along the dimension named above; an argument that names none is the same for every part.
All inputs are finite; a program needn't handle non-finite values.
Results may differ from the reference program's by a relative error of at most 0.0112909.
Values are sent between devices in bfloat16 or wider.
A program may use at most 768 MiB of HBM per device.

```python
import jax
import jax.numpy as jnp
from jax import lax

BATCH_ROWS = 1
TOKENS = 256
LATENT_CHAN = 16
MODEL_WIDTH = 384
NUM_HEADS = 6
STAGES = 8
STAGE_BLOCKS = 1
NUM_STEPS = 32

LAYERS = STAGES * STAGE_BLOCKS
HEAD_DIM = MODEL_WIDTH // NUM_HEADS
LN_EPS = 1e-6


def setup_inputs(seed: int = 0, part: int = 0) -> dict:
    key_base = jax.random.key(seed)
    part_keys = jax.random.split(jax.random.fold_in(key_base, part), 2)
    shared_keys = jax.random.split(key_base, 8)
    model_width = MODEL_WIDTH
    x_init = jax.random.normal(part_keys[0], (BATCH_ROWS, TOKENS, LATENT_CHAN), jnp.float32)
    w_in = jax.random.normal(shared_keys[0], (LATENT_CHAN, model_width), jnp.float32) * LATENT_CHAN ** -0.5
    w_out = jax.random.normal(shared_keys[1], (model_width, LATENT_CHAN), jnp.float32) * model_width ** -0.5
    w_qkv = jax.random.normal(shared_keys[2], (LAYERS, model_width, 3 * model_width), jnp.float32) * model_width ** -0.5
    w_proj = jax.random.normal(shared_keys[3], (LAYERS, NUM_HEADS, HEAD_DIM, model_width), jnp.float32) * model_width ** -0.5
    w_up = jax.random.normal(shared_keys[4], (LAYERS, model_width, 4 * model_width), jnp.float32) * model_width ** -0.5
    w_down = jax.random.normal(shared_keys[5], (LAYERS, 4 * model_width, model_width), jnp.float32) * (4 * model_width) ** -0.5
    mod_scale = jnp.array([0.5, 0.3, 0.5, 0.5, 0.3, 0.5], jnp.float32)[:, None]
    mod_shift = jnp.array([0.0, 0.0, 0.4, 0.0, 0.0, 0.4], jnp.float32)[:, None]
    mod_table = jax.random.normal(shared_keys[6], (NUM_STEPS, LAYERS, 6, model_width), jnp.float32) * mod_scale + mod_shift
    coef_draw = jax.random.uniform(shared_keys[7], (2, NUM_STEPS), jnp.float32)
    coef_keep = 0.9 + 0.07 * coef_draw[0]
    coef_noise = 0.15 + 0.2 * coef_draw[1]
    h_warm = jax.random.normal(part_keys[1], (2, STAGES - 1, BATCH_ROWS, TOKENS, model_width), jnp.float32)
    return {
        'x_init': x_init,
        'w_in': w_in.astype(jnp.bfloat16),
        'w_out': w_out.astype(jnp.bfloat16),
        'w_qkv': w_qkv.astype(jnp.bfloat16),
        'w_proj': w_proj.astype(jnp.bfloat16),
        'w_up': w_up.astype(jnp.bfloat16),
        'w_down': w_down.astype(jnp.bfloat16),
        'mod_table': mod_table,
        'coef_keep': coef_keep,
        'coef_noise': coef_noise,
        'h_warm': h_warm.astype(jnp.bfloat16),
    }


def layer_norm(hidden):
    row_mean = jnp.mean(hidden, axis=-1, keepdims=True)
    centered = hidden - row_mean
    row_var = jnp.mean(centered * centered, axis=-1, keepdims=True)
    return centered * lax.rsqrt(row_var + LN_EPS)


def dense_apply(activation, weight):
    flat_act = activation.reshape(-1, weight.shape[0])
    out_flat = jnp.dot(flat_act, weight, preferred_element_type=jnp.float32)
    return out_flat.reshape(activation.shape[:-1] + (weight.shape[1],))


def dit_block(hidden, layer_args):
    w_qkv_l, w_proj_l, w_up_l, w_down_l, mod_l = layer_args
    batch_rows = hidden.shape[0]
    normed = layer_norm(hidden) * (1.0 + mod_l[1]) + mod_l[0]
    qkv_all = dense_apply(normed.astype(jnp.bfloat16), w_qkv_l).astype(jnp.bfloat16)
    qkv_all = qkv_all.reshape(batch_rows, TOKENS, 3, NUM_HEADS, HEAD_DIM).astype(jnp.float32)
    scores = jnp.einsum('bqhd,bkhd->bhqk', qkv_all[:, :, 0], qkv_all[:, :, 1]) * HEAD_DIM ** -0.5
    attn_prob = jax.nn.softmax(scores, axis=-1).astype(jnp.bfloat16).astype(jnp.float32)
    attn_out = jnp.einsum('bhqk,bkhd->bqhd', attn_prob, qkv_all[:, :, 2]).astype(jnp.bfloat16)
    attn_flat = attn_out.reshape(batch_rows, TOKENS, MODEL_WIDTH)
    proj_weight = w_proj_l.reshape(MODEL_WIDTH, MODEL_WIDTH)
    hidden = hidden + mod_l[2] * dense_apply(attn_flat, proj_weight)
    normed = layer_norm(hidden) * (1.0 + mod_l[4]) + mod_l[3]
    mlp_act = jax.nn.gelu(dense_apply(normed.astype(jnp.bfloat16), w_up_l)).astype(jnp.bfloat16)
    hidden = hidden + mod_l[5] * dense_apply(mlp_act, w_down_l)
    return hidden, None


def run_stage(stage_args):
    hidden, _ = lax.scan(dit_block, stage_args[0], stage_args[1:])
    return hidden


def by_stage(weight):
    return weight.reshape((STAGES, STAGE_BLOCKS) + weight.shape[1:])


def reference(x_init, w_in, w_out, w_qkv, w_proj, w_up, w_down, mod_table, coef_keep, coef_noise, h_warm):
    stage_weights = (by_stage(w_qkv), by_stage(w_proj), by_stage(w_up), by_stage(w_down))

    def one_step(loop_state, step_idx):
        bound_now, bound_next, lat_now, x_cur = loop_state
        embedded = dense_apply(lat_now.astype(jnp.bfloat16), w_in)
        stage_in = jnp.concatenate([embedded[None], bound_now.astype(jnp.float32)], axis=0)
        mod_step = by_stage(mod_table[step_idx])
        stage_out = lax.map(run_stage, (stage_in,) + stage_weights + (mod_step,))
        normed = layer_norm(stage_out[STAGES - 1]).astype(jnp.bfloat16)
        noise_pred = dense_apply(normed, w_out)
        x_next = coef_keep[step_idx] * x_cur + coef_noise[step_idx] * noise_pred
        new_bound = stage_out[: STAGES - 1].astype(jnp.bfloat16)
        return (bound_next, new_bound, x_cur, x_next), None

    init_state = (h_warm[0], h_warm[1], x_init, x_init)
    final_state, _ = lax.scan(one_step, init_state, jnp.arange(NUM_STEPS))
    return final_state[3]
```

```python
import functools
import math

import jax
import jax.numpy as jnp
from jax import lax
from jax.experimental import pallas as pl
from jax.experimental.pallas import tpu as pltpu
from jax.sharding import PartitionSpec as P

LN_EPS = 1e-6
LOG2E = math.log2(math.e)
GELU_A = math.sqrt(2.0 / math.pi)
GELU_B = GELU_A * 0.044715


def normalize(hidden):
    scale = 1.0 / hidden.shape[0]
    mean = jnp.sum(hidden, axis=0, keepdims=True) * scale
    centered = hidden - mean
    var = jnp.sum(centered * centered, axis=0, keepdims=True) * scale
    return centered * lax.rsqrt(var + LN_EPS)


def dot(lhs, rhs):
    return jnp.dot(lhs, rhs, preferred_element_type=jnp.float32)


def kernel(stages, blocks, x_ref, w_in_ref, w_out_ref, qkv_hbm, proj_hbm, up_hbm, down_hbm, mod_ref, keep_ref, noise_ref, warm_hbm,
           out_ref, qkv_n, proj_n, up_n, down_n, warm_n, w_in_t, qkv_w, proj_w, up_w, down_w,
           recv, sent, x_recv, x_cur, h_scr, u_scr, qkv_scr, o_scr, act_scr,
           load_sem, recv_sem, send_sem, x_recv_sem, x_send_sem, last_send_sem, last_recv_sem):
    stage = lax.axis_index('stage')
    is_first = stage == 0
    is_last = stage == stages - 1
    steps = keep_ref.shape[0]
    width, tokens = h_scr.shape
    heads, head_dim = proj_hbm.shape[0], proj_hbm.shape[1]
    bf16 = jnp.bfloat16

    loads = [
        pltpu.make_async_copy(warm_hbm.at[:, jnp.maximum(stage - 1, 0), 0], warm_n, load_sem.at[0]),
        pltpu.make_async_copy(qkv_hbm, qkv_n, load_sem.at[1]),
        pltpu.make_async_copy(proj_hbm, proj_n, load_sem.at[2]),
        pltpu.make_async_copy(up_hbm, up_n, load_sem.at[3]),
        pltpu.make_async_copy(down_hbm, down_n, load_sem.at[4]),
    ]
    for copy in loads:
        copy.start()
    barrier = pltpu.get_barrier_semaphore()
    for ahead in range(1, stages):
        pl.semaphore_signal(barrier, inc=1, device_id={'stage': lax.rem(stage + ahead, stages)},
                            device_id_type=pl.DeviceIdType.MESH)

    w_in_t[...] = w_in_ref[...].T
    x_cur[...] = x_ref[...]
    for slot in range(2):
        x_recv[slot] = x_ref[...]
    loads[0].wait()
    for slot in range(2):
        recv[slot] = warm_n[slot].T
    loads[1].wait()
    qkv_w[...] = qkv_n[...].T
    loads[2].wait()
    proj_w[...] = proj_n[...].reshape(width, width).T
    loads[3].wait()
    up_w[...] = up_n[...].T
    loads[4].wait()
    down_w[...] = down_n[...].T
    pl.semaphore_wait(barrier, stages - 1)

    next_id = {'stage': lax.rem(stage + 1, stages)}

    def hidden_copy(step):
        return pltpu.make_async_remote_copy(
            src_ref=sent.at[step], dst_ref=recv.at[step + 2], send_sem=send_sem.at[step], recv_sem=recv_sem.at[step + 2],
            device_id=next_id, device_id_type=pl.DeviceIdType.MESH)

    def latent_copy(step):
        return pltpu.make_async_remote_copy(
            src_ref=x_recv.at[step + 2], dst_ref=x_recv.at[step + 2], send_sem=x_send_sem.at[step], recv_sem=x_recv_sem.at[step + 2],
            device_id=next_id, device_id_type=pl.DeviceIdType.MESH)

    first_trips = steps - 2 * (stages - 1)
    trips = first_trips + 2 * stage

    def one_step(step, carry):
        @pl.when(is_first)
        def _():
            @pl.when(step >= 2)
            def _():
                latent_copy(step - 2).wait_recv()
            h_scr[...] = dot(w_in_t[...], x_recv[step].astype(bf16))

        @pl.when(jnp.logical_not(is_first))
        def _():
            @pl.when(step >= 2)
            def _():
                hidden_copy(step - 2).wait_recv()
            h_scr[...] = recv[step].astype(jnp.float32)

        mod_t = mod_ref[step].T
        parts = width // 128

        def mod_col(row, plus=0.0):
            cols = [mod_t[:, row * parts + part:row * parts + part + 1] for part in range(parts)]
            col = jnp.concatenate(cols, axis=0) + plus
            return jnp.broadcast_to(col, (width, tokens))

        hidden = h_scr[...]
        u_scr[...] = (normalize(hidden) * mod_col(1, 1.0) + mod_col(0)).astype(bf16)
        qkv_scr[...] = dot(qkv_w[...], u_scr[...]).astype(bf16)
        factor = LOG2E * head_dim ** -0.5
        for head in range(heads):
            lo = head * head_dim
            query = qkv_scr[lo:lo + head_dim]
            key = qkv_scr[width + lo:width + lo + head_dim]
            value = qkv_scr[2 * width + lo:2 * width + lo + head_dim]
            scores = dot(key.T, query)
            top = jnp.max(scores, axis=0, keepdims=True)
            expo = jnp.exp2((scores - top) * factor)
            total = jnp.sum(expo, axis=0, keepdims=True)
            o_scr[lo:lo + head_dim] = (dot(value, expo.astype(bf16)) * (1.0 / total)).astype(bf16)
        hidden = h_scr[...] + mod_col(2) * dot(proj_w[...], o_scr[...])
        h_scr[...] = hidden
        u_scr[...] = (normalize(hidden) * mod_col(4, 1.0) + mod_col(3)).astype(bf16)
        chunk = width
        for lo in range(0, 4 * width, chunk):
            pre = dot(up_w[lo:lo + chunk], u_scr[...])
            half = 0.5 * pre
            act_scr[lo:lo + chunk] = (half * jnp.tanh(pre * (GELU_A + GELU_B * (pre * pre))) + half).astype(bf16)
        hidden = h_scr[...] + mod_col(5) * dot(down_w[...], act_scr[...])

        @pl.when(jnp.logical_not(is_last))
        def _():
            sent[step] = hidden.astype(bf16)
            hidden_copy(step).start()

        @pl.when(is_last)
        def _():
            noise = dot(w_out_ref[...], normalize(hidden).astype(bf16))
            x_next = keep_ref[step] * x_cur[...] + noise_ref[step] * noise
            x_cur[...] = x_next

            @pl.when(step + 2 < first_trips)
            def _():
                x_recv[step + 2] = x_next
                latent_copy(step).start()
        return carry

    lax.fori_loop(0, trips, one_step, 0)

    def final_copy(ahead):
        return pltpu.make_async_remote_copy(
            src_ref=x_cur, dst_ref=out_ref, send_sem=last_send_sem.at[ahead], recv_sem=last_recv_sem,
            device_id={'stage': lax.rem(stage + ahead, stages)}, device_id_type=pl.DeviceIdType.MESH)

    @pl.when(is_last)
    def _():
        for ahead in range(1, stages):
            final_copy(ahead).start()
        out_ref[...] = x_cur[...]
        for ahead in range(1, stages):
            final_copy(ahead).wait_send()

        def drain(step, carry):
            latent_copy(step).wait_send()
            return carry
        lax.fori_loop(0, first_trips - 2, drain, 0)

    @pl.when(jnp.logical_not(is_last))
    def _():
        def drain(step, carry):
            hidden_copy(step).wait_send()
            return carry
        lax.fori_loop(0, trips, drain, 0)
        final_copy(1).wait_recv()


def solution(mesh):
    stages = mesh.shape['stage']

    def shard_body(x_init, w_in, w_out, w_qkv, w_proj, w_up, w_down, mod_table, coef_keep, coef_noise, h_warm):
        steps = coef_keep.shape[0]
        rows, tokens, chan = x_init.shape
        blocks, width = w_qkv.shape[0], w_qkv.shape[1]
        mlp = w_up.shape[2]
        heads, head_dim = w_proj.shape[1], w_proj.shape[2]
        bf16, f32 = jnp.bfloat16, jnp.float32
        vmem = pl.BlockSpec(memory_space=pltpu.VMEM)
        smem = pl.BlockSpec(memory_space=pltpu.SMEM)
        hbm = pl.BlockSpec(memory_space=pl.ANY)
        mod = mod_table.reshape(steps, 6 * width // 128, 128)
        mod = jnp.pad(mod, ((0, 0), (0, -mod.shape[1] % 8), (0, 0)))
        out = pl.pallas_call(
            functools.partial(kernel, stages, blocks),
            out_shape=jax.ShapeDtypeStruct((chan, tokens), f32),
            in_specs=[vmem, vmem, vmem, hbm, hbm, hbm, hbm, vmem, smem, smem, hbm],
            out_specs=vmem,
            scratch_shapes=[
                pltpu.VMEM((width, 3 * width), bf16),
                pltpu.VMEM((heads, head_dim, width), bf16),
                pltpu.VMEM((width, mlp), bf16),
                pltpu.VMEM((mlp, width), bf16),
                pltpu.VMEM((2, tokens, width), bf16),
                pltpu.VMEM((width, chan), bf16),
                pltpu.VMEM((3 * width, width), bf16),
                pltpu.VMEM((width, width), bf16),
                pltpu.VMEM((mlp, width), bf16),
                pltpu.VMEM((width, mlp), bf16),
                pltpu.VMEM((steps, width, tokens), bf16),
                pltpu.VMEM((steps, width, tokens), bf16),
                pltpu.VMEM((steps, chan, tokens), f32),
                pltpu.VMEM((chan, tokens), f32),
                pltpu.VMEM((width, tokens), f32),
                pltpu.VMEM((width, tokens), bf16),
                pltpu.VMEM((3 * width, tokens), bf16),
                pltpu.VMEM((width, tokens), bf16),
                pltpu.VMEM((mlp, tokens), bf16),
                pltpu.SemaphoreType.DMA((5,)),
                pltpu.SemaphoreType.DMA((steps,)),
                pltpu.SemaphoreType.DMA((steps,)),
                pltpu.SemaphoreType.DMA((steps,)),
                pltpu.SemaphoreType.DMA((steps,)),
                pltpu.SemaphoreType.DMA((stages,)),
                pltpu.SemaphoreType.DMA,
            ],
            compiler_params=pltpu.CompilerParams(collective_id=0, has_side_effects=True, vmem_limit_bytes=56 * 1024 * 1024),
            name='stage_loop',
        )(jnp.swapaxes(x_init, 1, 2)[0], w_in, jnp.swapaxes(w_out, 0, 1), w_qkv[0], w_proj[0], w_up[0], w_down[0], mod,
          coef_keep, coef_noise, h_warm)
        return jnp.swapaxes(out, 0, 1)[None]

    return jax.shard_map(
        shard_body,
        mesh=mesh,
        in_specs=(P('data'), P(), P(), P('stage'), P('stage'), P('stage'), P('stage'), P(None, 'stage'), P(), P(), P(None, None, 'data')),
        out_specs=P('data'),
        check_vma=False,
    )
```

```python
import functools
import math

import jax
import jax.numpy as jnp
from jax import lax
from jax.experimental import pallas as pl
from jax.experimental.pallas import tpu as pltpu
from jax.sharding import PartitionSpec as P

LN_EPS = 1e-6
LOG2E = math.log2(math.e)
GELU_A = math.sqrt(2.0 / math.pi)
GELU_B = GELU_A * 0.044715
CHUNK = 256
MESH = pl.DeviceIdType.MESH


def fold(rows):
    while rows.shape[0] % 16 == 0:
        half = rows.shape[0] // 2
        rows = rows[:half] + rows[half:]
    parts = [rows[lo:lo + 8] for lo in range(0, rows.shape[0], 8)]
    while len(parts) > 1:
        parts = [a + b for a, b in zip(parts[::2], parts[1::2])] + parts[len(parts) - len(parts) % 2:]
    return jnp.sum(parts[0], axis=0, keepdims=True)


def normalize(hidden):
    scale = 1.0 / hidden.shape[0]
    centered = hidden - fold(hidden) * scale
    var = fold(centered * centered) * scale
    return centered * lax.rsqrt(var + LN_EPS)


def dot(lhs, rhs):
    return jnp.dot(lhs, rhs, preferred_element_type=jnp.float32)


def kernel(stages, x_ref, w_in_ref, w_out_ref, qkv_hbm, proj_hbm, up_hbm, down_hbm, mod_ref, keep_ref, noise_ref, warm_hbm,
           out_ref, qkv_n, proj_n, up_n, down_n, warm_n, w_in_t, qkv_w, proj_w, up_w, down_w, mod_s, select, lanes,
           recv, sent, x_recv, x_cur, h_last, h_scr, u_scr, o_scr, load_sem, recv_sem, send_sem, x_recv_sem, x_send_sem, last_send_sem, last_recv_sem):
    stage = lax.axis_index('stage')
    is_first = stage == 0
    is_last = stage == stages - 1
    steps = keep_ref.shape[0]
    width, tokens = h_last.shape
    heads, head_dim = proj_hbm.shape[0], proj_hbm.shape[1]
    mlp = up_w.shape[0]
    lanes_k = select.shape[1]
    bf16, f32 = jnp.bfloat16, jnp.float32

    loads = [
        pltpu.make_async_copy(warm_hbm.at[:, jnp.maximum(stage - 1, 0), 0], warm_n, load_sem.at[0]),
        pltpu.make_async_copy(qkv_hbm, qkv_n, load_sem.at[1]),
        pltpu.make_async_copy(proj_hbm, proj_n, load_sem.at[2]),
        pltpu.make_async_copy(up_hbm, up_n, load_sem.at[3]),
        pltpu.make_async_copy(down_hbm, down_n, load_sem.at[4]),
    ]
    for copy in loads:
        copy.start()
    barrier = pltpu.get_barrier_semaphore()
    for ahead in range(1, stages):
        pl.semaphore_signal(barrier, inc=1, device_id={'stage': lax.rem(stage + ahead, stages)}, device_id_type=MESH)

    mod_rows = mod_ref.shape[0] // steps
    parts = width // 128
    pad = lanes_k // 3
    row_id = lax.broadcasted_iota(jnp.int32, (mod_rows, 128), 0) // parts
    plus = jnp.where((row_id == 1) | (row_id == 4), 1.0, 0.0)
    limit = float(jnp.finfo(bf16).max)
    gap = jnp.zeros((pad - mod_rows, 128), f32)

    def split_mod(step, carry):
        rows = mod_ref[pl.ds(step * mod_rows, mod_rows)] + plus
        high = jnp.clip(rows, -limit, limit).astype(bf16).astype(f32)
        rest = rows - high
        mid = rest.astype(bf16).astype(f32)
        terms = jnp.concatenate([high, gap, mid, gap, rest - mid, gap], axis=0)
        mod_s[step] = terms.T.astype(bf16)
        return carry

    lax.fori_loop(0, steps, split_mod, 0)
    term = lax.broadcasted_iota(jnp.int32, (lanes_k, 256), 0) % pad
    column = lax.broadcasted_iota(jnp.int32, (lanes_k, 256), 1) // 128
    for pair in range(3):
        for part in range(parts):
            pick = term == (2 * pair + column) * parts + part
            select[pair * parts + part] = jnp.where(pick, 1.0, 0.0).astype(bf16)

    def fill_lanes(step, pair, part):
        both = dot(mod_s[step], select[pair * parts + part])
        for side in range(2):
            lanes[2 * pair + side, part * 128:part * 128 + 128] = both[:, side * 128:side * 128 + 128]

    halves = [slice(lo, lo + 128) for lo in range(0, tokens, 128)]

    w_in_t[...] = w_in_ref[...].T
    x_cur[...] = x_ref[...]
    for slot in range(2):
        x_recv[slot] = x_ref[...]
    loads[0].wait()
    for slot in range(2):
        recv[slot] = warm_n[slot].T
    loads[1].wait()
    qkv_w[...] = qkv_n[...].T
    loads[2].wait()
    proj_w[...] = proj_n[...].reshape(width, width).T
    loads[3].wait()
    up_w[...] = up_n[...].T * jnp.asarray(0.5, bf16)
    loads[4].wait()
    down_w[...] = down_n[...].T
    pl.semaphore_wait(barrier, stages - 1)

    next_id = {'stage': lax.rem(stage + 1, stages)}

    def hidden_copy(step):
        return pltpu.make_async_remote_copy(
            src_ref=sent.at[step], dst_ref=recv.at[step + 2], send_sem=send_sem.at[step], recv_sem=recv_sem.at[step + 2],
            device_id=next_id, device_id_type=MESH)

    def latent_copy(step):
        return pltpu.make_async_remote_copy(
            src_ref=x_recv.at[step + 2], dst_ref=x_recv.at[step + 2], send_sem=x_send_sem.at[step], recv_sem=x_recv_sem.at[step + 2],
            device_id=next_id, device_id_type=MESH)

    first_trips = steps - 2 * (stages - 1)
    trips = first_trips + 2 * stage

    def norm_into(hidden, scale_row, shift_row, half):
        u_scr[:, half] = (normalize(hidden) * lanes[scale_row] + lanes[shift_row]).astype(bf16)

    def block(step, hidden_in, beside=lambda: None):
        for part in range(parts):
            fill_lanes(step, 0, part)
        for half in halves:
            norm_into(hidden_in(half), 1, 0, half)
        normed = u_scr[...]
        key = dot(qkv_w[width:2 * width], normed).astype(bf16)
        query = dot(qkv_w[:width], normed).astype(bf16)
        factor = LOG2E * head_dim ** -0.5

        def head(rows, index):
            return rows[index * head_dim:(index + 1) * head_dim]

        def score(index):
            return dot(head(key, index).T, head(query, index))

        def softmax(scores):
            top = jnp.max(scores, axis=0, keepdims=True)
            expo = jnp.exp2((scores - top) * factor)
            return expo.astype(bf16), 1.0 / fold(expo)

        scores = {0: score(0), 1: score(1)}
        value = dot(qkv_w[2 * width:], normed).astype(bf16)
        fills = [(pair, part) for pair in (1, 2) for part in range(parts)]
        split = 256 // head_dim
        proj = [None, None]
        mid = width // 2

        def project(lo, hi):
            rows = o_scr[lo:hi]
            for side in range(2):
                piece = dot(proj_w[side * mid:side * mid + mid, lo:hi], rows)
                proj[side] = piece if proj[side] is None else proj[side] + piece

        for index in range(heads):
            if index + 2 < heads:
                scores[index + 2] = score(index + 2)
            cur = scores.pop(index)
            done = [softmax(cur[:, half]) for half in halves]
            expo = jnp.concatenate([pair[0] for pair in done], axis=1)
            inverse = jnp.concatenate([pair[1] for pair in done], axis=1)
            o_scr[index * head_dim:(index + 1) * head_dim] = (dot(head(value, index), expo) * inverse).astype(bf16)
            if index < len(fills):
                fill_lanes(step, *fills[index])
            if index == 0:
                beside()
            if index == split - 1:
                project(0, 256)
        project(256, width)
        for half in halves:
            hidden = hidden_in(half) + lanes[2] * jnp.concatenate([side[:, half] for side in proj], axis=0)
            h_scr[:, half] = hidden
            norm_into(hidden, 4, 3, half)
        normed = u_scr[...]
        count = mlp // CHUNK
        ups = {}

        def up(index):
            return dot(up_w[index * CHUNK:(index + 1) * CHUNK], normed)

        ups[0] = up(0)
        total = [None, None]
        for index in range(count):
            if index + 1 < count:
                ups[index + 1] = up(index + 1)
            pre = ups.pop(index)
            act = (pre * jnp.tanh(pre * (2.0 * GELU_A + 8.0 * GELU_B * (pre * pre))) + pre).astype(bf16)
            for side in range(2):
                piece = dot(down_w[side * mid:side * mid + mid, index * CHUNK:(index + 1) * CHUNK], act)
                total[side] = piece if total[side] is None else total[side] + piece
        for half in halves:
            yield half, h_scr[:, half] + lanes[5] * jnp.concatenate([side[:, half] for side in total], axis=0)

    def send(step, columns):
        for half, hidden in columns:
            sent[step, :, half] = hidden.astype(bf16)
        hidden_copy(step).start()

    def received(step):
        return lambda half: recv[step, :, half].astype(f32)

    def wait_hidden(step):
        @pl.when(step >= 2)
        def _():
            hidden_copy(step - 2).wait_recv()

    def first_step(step, carry):
        @pl.when(step >= 2)
        def _():
            latent_copy(step - 2).wait_recv()
        embedded = dot(w_in_t[...], x_recv[step].astype(bf16))
        h_last[...] = embedded
        send(step, block(step, lambda half: h_last[:, half]))
        return carry

    def middle_step(step, carry):
        wait_hidden(step)
        send(step, block(step, received(step)))
        return carry

    def advance(step):
        normed = jnp.concatenate([normalize(h_last[:, half]).astype(bf16) for half in halves], axis=1)
        noise = dot(w_out_ref[...], normed)
        x_next = keep_ref[step] * x_cur[...] + noise_ref[step] * noise
        x_cur[...] = x_next
        return x_next

    def last_step(step, carry):
        wait_hidden(step)
        before = jnp.maximum(step - 1, 0)

        def beside():
            x_next = jnp.where(step > 0, advance(before), x_ref[...])
            x_cur[...] = x_next
            x_recv[jnp.minimum(before + 2, steps - 1)] = x_next

        for half, hidden in block(step, received(step), beside):
            h_last[:, half] = hidden

        @pl.when((step > 0) & (before + 2 < first_trips))
        def _():
            latent_copy(before).start()
        return carry

    def final_copy(ahead):
        return pltpu.make_async_remote_copy(
            src_ref=x_cur, dst_ref=out_ref, send_sem=last_send_sem.at[ahead], recv_sem=last_recv_sem,
            device_id={'stage': lax.rem(stage + ahead, stages)}, device_id_type=MESH)

    @pl.when(is_first)
    def _():
        lax.fori_loop(0, first_trips, first_step, 0)

    @pl.when(jnp.logical_not(is_first | is_last))
    def _():
        lax.fori_loop(0, trips, middle_step, 0)

    @pl.when(is_last)
    def _():
        h_last[...] = jnp.zeros_like(h_last)
        lax.fori_loop(0, steps, last_step, 0)
        out_ref[...] = advance(steps - 1)
        for ahead in range(1, stages):
            final_copy(ahead).start()
        for ahead in range(1, stages):
            final_copy(ahead).wait_send()

        def drain(step, carry):
            latent_copy(step).wait_send()
            return carry
        lax.fori_loop(0, first_trips - 2, drain, 0)

    @pl.when(jnp.logical_not(is_last))
    def _():
        def drain(step, carry):
            hidden_copy(step).wait_send()
            return carry
        lax.fori_loop(0, trips, drain, 0)
        final_copy(1).wait_recv()


def solution(mesh):
    stages = mesh.shape['stage']

    def shard_body(x_init, w_in, w_out, w_qkv, w_proj, w_up, w_down, mod_table, coef_keep, coef_noise, h_warm):
        steps = coef_keep.shape[0]
        tokens, chan = x_init.shape[1], x_init.shape[2]
        width, mlp = w_up.shape[1], w_up.shape[2]
        heads, head_dim = w_proj.shape[1], w_proj.shape[2]
        mod_rows = mod_table.shape[2] * width // 128
        lanes_k = 3 * (mod_rows + -mod_rows % 8)
        bf16, f32 = jnp.bfloat16, jnp.float32
        vmem = pl.BlockSpec(memory_space=pltpu.VMEM)
        smem = pl.BlockSpec(memory_space=pltpu.SMEM)
        hbm = pl.BlockSpec(memory_space=pl.ANY)
        out = pl.pallas_call(
            functools.partial(kernel, stages),
            out_shape=jax.ShapeDtypeStruct((chan, tokens), f32),
            in_specs=[vmem, vmem, vmem, hbm, hbm, hbm, hbm, vmem, smem, smem, hbm],
            out_specs=vmem,
            scratch_shapes=[
                pltpu.VMEM((width, 3 * width), bf16),
                pltpu.VMEM((heads, head_dim, width), bf16),
                pltpu.VMEM((width, mlp), bf16),
                pltpu.VMEM((mlp, width), bf16),
                pltpu.VMEM((2, tokens, width), bf16),
                pltpu.VMEM((width, chan), bf16),
                pltpu.VMEM((3 * width, width), bf16),
                pltpu.VMEM((width, width), bf16),
                pltpu.VMEM((mlp, width), bf16),
                pltpu.VMEM((width, mlp), bf16),
                pltpu.VMEM((steps, 128, lanes_k), bf16),
                pltpu.VMEM((3 * width // 128, lanes_k, 256), bf16),
                pltpu.VMEM((6, width, 128), f32),
                pltpu.VMEM((steps, width, tokens), bf16),
                pltpu.VMEM((steps, width, tokens), bf16),
                pltpu.VMEM((steps, chan, tokens), f32),
                pltpu.VMEM((chan, tokens), f32),
                pltpu.VMEM((width, tokens), f32),
                pltpu.VMEM((width, tokens), f32),
                pltpu.VMEM((width, tokens), bf16),
                pltpu.VMEM((width, tokens), bf16),
                pltpu.SemaphoreType.DMA((5,)),
                pltpu.SemaphoreType.DMA((steps,)),
                pltpu.SemaphoreType.DMA((steps,)),
                pltpu.SemaphoreType.DMA((steps,)),
                pltpu.SemaphoreType.DMA((steps,)),
                pltpu.SemaphoreType.DMA((stages,)),
                pltpu.SemaphoreType.DMA,
            ],
            compiler_params=pltpu.CompilerParams(collective_id=0, has_side_effects=True, vmem_limit_bytes=56 * 1024 * 1024),
            name='stage_loop',
        )(jnp.swapaxes(x_init, 1, 2)[0], w_in, jnp.swapaxes(w_out, 0, 1), w_qkv[0], w_proj[0], w_up[0], w_down[0],
          mod_table.reshape(steps * mod_rows, 128), coef_keep, coef_noise, h_warm)
        return jnp.swapaxes(out, 0, 1)[None]

    return jax.shard_map(
        shard_body,
        mesh=mesh,
        in_specs=(P('data'), P(), P(), P('stage'), P('stage'), P('stage'), P('stage'), P(None, 'stage'), P(), P(), P(None, None, 'data')),
        out_specs=P('data'),
        check_vma=False,
    )
```

```python
import functools
import math

import jax
import jax.numpy as jnp
from jax import lax
from jax.experimental import pallas as pl
from jax.experimental.pallas import tpu as pltpu
from jax.sharding import PartitionSpec as P

LN_EPS = 1e-6
LOG2E = math.log2(math.e)
GELU_A = math.sqrt(2.0 / math.pi)
GELU_B = GELU_A * 0.044715
UNIT = 64
MESH = pl.DeviceIdType.MESH


def fold(rows):
    while rows.shape[0] % 16 == 0:
        half = rows.shape[0] // 2
        rows = rows[:half] + rows[half:]
    parts = [rows[lo:lo + 8] for lo in range(0, rows.shape[0], 8)]
    while len(parts) > 1:
        parts = [a + b for a, b in zip(parts[::2], parts[1::2])] + parts[len(parts) - len(parts) % 2:]
    return jnp.sum(parts[0], axis=0, keepdims=True)


def normalize(hidden):
    scale = 1.0 / hidden.shape[0]
    centered = hidden - fold(hidden) * scale
    var = fold(centered * centered) * scale
    return centered * lax.rsqrt(var + LN_EPS)


def dot(lhs, rhs):
    return jnp.dot(lhs, rhs, preferred_element_type=jnp.float32)


def kernel(stages, x_ref, w_in_ref, w_out_ref, qkv_hbm, proj_hbm, up_hbm, down_hbm, mod_ref, keep_ref, noise_ref, warm_hbm,
           out_ref, qkv_n, proj_n, up_n, down_n, warm_n, w_in_t, qkv_w, proj_w, up_w, down_w, mod_s, select, lanes,
           recv, sent, x_recv, x_cur, h_last, h_scr, u_scr, o_scr, load_sem, recv_sem, send_sem, x_recv_sem, x_send_sem, last_send_sem, last_recv_sem):
    stage = lax.axis_index('stage')
    is_first = stage == 0
    is_last = stage == stages - 1
    steps = keep_ref.shape[0]
    width, tokens = h_last.shape
    heads, head_dim = proj_hbm.shape[0], proj_hbm.shape[1]
    mlp = up_w.shape[0]
    bf16, f32 = jnp.bfloat16, jnp.float32

    loads = [
        pltpu.make_async_copy(warm_hbm.at[:, jnp.maximum(stage - 1, 0), 0], warm_n, load_sem.at[0]),
        pltpu.make_async_copy(qkv_hbm, qkv_n, load_sem.at[1]),
        pltpu.make_async_copy(proj_hbm, proj_n, load_sem.at[2]),
        pltpu.make_async_copy(up_hbm, up_n, load_sem.at[3]),
        pltpu.make_async_copy(down_hbm, down_n, load_sem.at[4]),
    ]
    for copy in loads:
        copy.start()
    barrier = pltpu.get_barrier_semaphore()
    for ahead in range(1, stages):
        pl.semaphore_signal(barrier, inc=1, device_id={'stage': lax.rem(stage + ahead, stages)}, device_id_type=MESH)

    mod_rows = mod_ref.shape[0] // steps
    parts = width // 128
    pad = mod_rows + -mod_rows % 8
    row_id = lax.broadcasted_iota(jnp.int32, (mod_rows, 128), 0) // parts
    plus = jnp.where((row_id == 1) | (row_id == 4), 1.0, 0.0)
    limit = float(jnp.finfo(bf16).max)
    gap = jnp.zeros((pad - mod_rows, 128), f32)
    rest_rows = jnp.zeros((128 - 3 * pad, 128), f32)

    def split_mod(step, carry):
        rows = mod_ref[pl.ds(step * mod_rows, mod_rows)] + plus
        high = jnp.clip(rows, -limit, limit).astype(bf16).astype(f32)
        rest = rows - high
        mid = rest.astype(bf16).astype(f32)
        terms = jnp.concatenate([high, gap, mid, gap, rest - mid, gap, rest_rows], axis=0)
        mod_s[step] = terms.T.astype(bf16)
        return carry

    lax.fori_loop(0, steps, split_mod, 0)
    term = lax.broadcasted_iota(jnp.int32, (128, 256), 0)
    term = jnp.where(term < 3 * pad, term % pad, -1)
    column = lax.broadcasted_iota(jnp.int32, (128, 256), 1) // 128
    for pair in range(3):
        for part in range(parts):
            pick = term == (2 * pair + column) * parts + part
            select[pair * parts + part] = jnp.where(pick, 1.0, 0.0).astype(bf16)

    def fill(step, pair, part):
        return dot(mod_s[step], select[pair * parts + part])

    def store_fill(pair, part, both):
        for side in range(2):
            lanes[2 * pair + side, part * 128:part * 128 + 128] = both[:, side * 128:side * 128 + 128]

    halves = [slice(lo, lo + 128) for lo in range(0, tokens, 128)]

    w_in_t[...] = w_in_ref[...].T
    x_cur[...] = x_ref[...]
    for slot in range(2):
        x_recv[slot] = x_ref[...]
    loads[0].wait()
    for slot in range(2):
        recv[slot] = warm_n[slot].T
    loads[1].wait()
    qkv_w[...] = qkv_n[...].T
    loads[2].wait()
    proj_w[...] = proj_n[...].reshape(width, width).T
    loads[3].wait()
    up_w[...] = up_n[...].T * jnp.asarray(0.5, bf16)
    loads[4].wait()
    down_w[...] = down_n[...].T
    for part in range(parts):
        store_fill(0, part, fill(0, 0, part))
    pl.semaphore_wait(barrier, stages - 1)

    next_id = {'stage': lax.rem(stage + 1, stages)}

    def hidden_copy(step):
        return pltpu.make_async_remote_copy(
            src_ref=sent.at[step], dst_ref=recv.at[step + 2], send_sem=send_sem.at[step], recv_sem=recv_sem.at[step + 2],
            device_id=next_id, device_id_type=MESH)

    def latent_copy(step):
        return pltpu.make_async_remote_copy(
            src_ref=x_recv.at[step + 2], dst_ref=x_recv.at[step + 2], send_sem=x_send_sem.at[step], recv_sem=x_recv_sem.at[step + 2],
            device_id=next_id, device_id_type=MESH)

    first_trips = steps - 2 * (stages - 1)
    trips = first_trips + 2 * stage

    row_units = [slice(lo, lo + UNIT) for lo in range(0, width, UNIT)]

    def to_tile(rows):
        while rows.shape[0] > 8:
            mid = rows.shape[0] // 2
            rows = rows[:mid] + rows[mid:]
        return rows

    def mean_of(tiles_of_half):
        total = tiles_of_half[0::2]
        total = [a + b for a, b in zip(total, tiles_of_half[1::2])]
        while len(total) > 1:
            total = [a + b for a, b in zip(total[::2], total[1::2])] + total[len(total) - len(total) % 2:]
        return jnp.sum(total[0], axis=0, keepdims=True) * (1.0 / width)

    def norm_store(sums, scale_row, shift_row):
        stats = []
        for half, tiles_of_half in zip(halves, sums):
            mean = mean_of(tiles_of_half)
            squares = []
            for rows in row_units:
                centered = h_scr[rows, half] - mean
                squares.append(to_tile(centered * centered))
            stats.append((mean, lax.rsqrt(mean_of(squares) + LN_EPS)))
        for rows in row_units:
            for half, (mean, rstd) in zip(halves, stats):
                u_scr[rows, half] = ((h_scr[rows, half] - mean) * rstd * lanes[scale_row, rows] + lanes[shift_row, rows]).astype(bf16)

    quarter = width // 2
    each = quarter // UNIT

    row_units = [slice(lo, lo + UNIT) for lo in range(0, width, UNIT)]

    def to_tile(rows):
        while rows.shape[0] > 8:
            mid = rows.shape[0] // 2
            rows = rows[:mid] + rows[mid:]
        return rows

    def mean_of(tiles_of_half):
        total = tiles_of_half[0::2]
        total = [a + b for a, b in zip(total, tiles_of_half[1::2])]
        while len(total) > 1:
            total = [a + b for a, b in zip(total[::2], total[1::2])] + total[len(total) - len(total) % 2:]
        return jnp.sum(total[0], axis=0, keepdims=True) * (1.0 / width)

    def norm_store(sums, scale_row, shift_row):
        stats = []
        for half, tiles_of_half in zip(halves, sums):
            mean = mean_of(tiles_of_half)
            squares = []
            for rows in row_units:
                centered = h_scr[rows, half] - mean
                squares.append(to_tile(centered * centered))
            stats.append((mean, lax.rsqrt(mean_of(squares) + LN_EPS)))
        for rows in row_units:
            for half, (mean, rstd) in zip(halves, stats):
                u_scr[rows, half] = ((h_scr[rows, half] - mean) * rstd * lanes[scale_row, rows] + lanes[shift_row, rows]).astype(bf16)

    quarter = width // 2
    each = quarter // UNIT

    def tiles(rows):
        return rows[:256], jnp.concatenate([zeros_half, rows[256:]], axis=0)

    def weight(ref, row, register):
        lo = 0 if register == 0 else width - 256
        return ref[row:row + UNIT, lo:lo + 256]

    def block(step, hidden_in, beside=lambda: None):
        fills = {(pair, part): fill(step, pair, part) for pair in (1, 2) for part in range(parts)}
        sums = [[], []]
        for rows in row_units:
            for side, half in enumerate(halves):
                hidden = hidden_in(half, rows)
                h_scr[rows, half] = hidden
                sums[side].append(to_tile(hidden))
        norm_store(sums, 1, 0)
        normed = u_scr[...]
        pairs = heads // 2

        def project_in(kind, lo, hi):
            start = kind * width
            return dot(qkv_w[start + lo * head_dim:start + hi * head_dim], normed).astype(bf16)

        def per_head(rows):
            return [rows[lo:lo + head_dim] for lo in range(0, rows.shape[0], head_dim)]

        groups = ((0, 2), (2, heads))
        keys, queries = [], []
        for lo, hi in groups:
            keys += per_head(project_in(1, lo, hi))
            queries += per_head(project_in(0, lo, hi))
        for (pair, part), both in fills.items():
            store_fill(pair, part, both)
        factor = LOG2E * head_dim ** -0.5

        def score(index):
            return [dot(keys[head].T, queries[head]) for head in (2 * index, 2 * index + 1)]

        def softmax(scores):
            top = jnp.max(scores, axis=0, keepdims=True)
            expo = jnp.exp2((scores - top) * factor)
            return expo.astype(bf16), 1.0 / fold(expo)

        scores = [score(0)]
        values = per_head(project_in(2, 0, heads // 2)) + per_head(project_in(2, heads // 2, heads))
        proj = [None, None]

        def project_out(lo, hi):
            for side in range(2):
                piece = dot(proj_w[side * quarter:side * quarter + quarter, lo:hi], o_scr[lo:hi])
                proj[side] = piece if proj[side] is None else proj[side] + piece

        for index in range(pairs):
            if index + 1 < pairs:
                scores.append(score(index + 1))
            for unit in range(2):
                head = 2 * index + unit
                done = [softmax(scores[index][unit][:, half]) for half in halves]
                inverse = jnp.concatenate([pair[1] for pair in done], axis=1)
                expo = jnp.concatenate([pair[0] for pair in done], axis=1)
                o_scr[head * head_dim:(head + 1) * head_dim] = (dot(values[head], expo) * inverse).astype(bf16)
            if index == 0:
                beside()
            if index == 1:
                project_out(0, 256)
        project_out(256, width)
        sums = [[], []]
        for unit in range(2):
            for part in range(each):
                lo = unit * quarter + part * UNIT
                rows = slice(lo, lo + UNIT)
                piece = proj[unit][part * UNIT:part * UNIT + UNIT]
                for side, half in enumerate(halves):
                    hidden = h_scr[rows, half] + lanes[2, rows] * piece[:, half]
                    h_scr[rows, half] = hidden
                    sums[side].append(to_tile(hidden))
        norm_store(sums, 4, 3)
        normed = u_scr[...]
        tile_count = mlp // 256
        ups = [dot(up_w[tile * 256:tile * 256 + 256], normed) for tile in range(tile_count)]

        def gelu(pre):
            return (pre * jnp.tanh(pre * (2.0 * GELU_A + 8.0 * GELU_B * (pre * pre))) + pre).astype(bf16)

        after = jnp.minimum(step + 1, steps - 1)
        down = [None, None]
        for tile in range(tile_count):
            act = jnp.concatenate([gelu(ups[tile][lo:lo + UNIT]) for lo in range(0, 256, UNIT)], axis=0)
            if tile == tile_count - 1:
                for part in range(parts):
                    store_fill(0, part, fill(after, 0, part))
            for side in range(2):
                piece = dot(down_w[side * quarter:side * quarter + quarter, tile * 256:tile * 256 + 256], act)
                down[side] = piece if down[side] is None else down[side] + piece
        for unit in range(2):
            for part in range(each):
                lo = unit * quarter + part * UNIT
                rows = slice(lo, lo + UNIT)
                for half in halves:
                    yield rows, half, h_scr[rows, half] + lanes[5, rows] * down[unit][part * UNIT:part * UNIT + UNIT, half]

    def send(step, columns):
        for rows, half, hidden in columns:
            sent[step, rows, half] = hidden.astype(bf16)
        hidden_copy(step).start()

    def received(step):
        return lambda half, rows=slice(None): recv[step, rows, half].astype(f32)

    def wait_hidden(step):
        @pl.when(step >= 2)
        def _():
            hidden_copy(step - 2).wait_recv()

    def first_step(step, carry):
        @pl.when(step >= 2)
        def _():
            latent_copy(step - 2).wait_recv()
        h_last[...] = dot(w_in_t[...], x_recv[step].astype(bf16))
        send(step, block(step, lambda half, rows=slice(None): h_last[rows, half]))
        return carry

    def middle_step(step, carry):
        wait_hidden(step)
        send(step, block(step, received(step)))
        return carry

    def advance(step):
        normed = jnp.concatenate([normalize(h_last[:, half]).astype(bf16) for half in halves], axis=1)
        noise = dot(w_out_ref[...], normed)
        x_next = keep_ref[step] * x_cur[...] + noise_ref[step] * noise
        x_cur[...] = x_next
        return x_next

    def last_step(step, carry):
        wait_hidden(step)
        before = jnp.maximum(step - 1, 0)

        def beside():
            x_next = jnp.where(step > 0, advance(before), x_ref[...])
            x_cur[...] = x_next
            x_recv[jnp.minimum(before + 2, steps - 1)] = x_next

        for rows, half, hidden in block(step, received(step), beside):
            h_last[rows, half] = hidden

        @pl.when((step > 0) & (before + 2 < first_trips))
        def _():
            latent_copy(before).start()
        return carry

    def final_copy(ahead):
        return pltpu.make_async_remote_copy(
            src_ref=x_cur, dst_ref=out_ref, send_sem=last_send_sem.at[ahead], recv_sem=last_recv_sem,
            device_id={'stage': lax.rem(stage + ahead, stages)}, device_id_type=MESH)

    @pl.when(is_first)
    def _():
        lax.fori_loop(0, first_trips, first_step, 0)

    @pl.when(jnp.logical_not(is_first | is_last))
    def _():
        lax.fori_loop(0, trips, middle_step, 0)

    @pl.when(is_last)
    def _():
        h_last[...] = jnp.zeros_like(h_last)
        lax.fori_loop(0, steps, last_step, 0)
        out_ref[...] = advance(steps - 1)
        for ahead in range(1, stages):
            final_copy(ahead).start()
        for ahead in range(1, stages):
            final_copy(ahead).wait_send()

        def drain(step, carry):
            latent_copy(step).wait_send()
            return carry
        lax.fori_loop(0, first_trips - 2, drain, 0)

    @pl.when(jnp.logical_not(is_last))
    def _():
        def drain(step, carry):
            hidden_copy(step).wait_send()
            return carry
        lax.fori_loop(0, trips, drain, 0)
        final_copy(1).wait_recv()


def solution(mesh):
    stages = mesh.shape['stage']

    def shard_body(x_init, w_in, w_out, w_qkv, w_proj, w_up, w_down, mod_table, coef_keep, coef_noise, h_warm):
        steps = coef_keep.shape[0]
        tokens, chan = x_init.shape[1], x_init.shape[2]
        width, mlp = w_up.shape[1], w_up.shape[2]
        heads, head_dim = w_proj.shape[1], w_proj.shape[2]
        mod_rows = mod_table.shape[2] * width // 128
        bf16, f32 = jnp.bfloat16, jnp.float32
        vmem = pl.BlockSpec(memory_space=pltpu.VMEM)
        smem = pl.BlockSpec(memory_space=pltpu.SMEM)
        hbm = pl.BlockSpec(memory_space=pl.ANY)
        out = pl.pallas_call(
            functools.partial(kernel, stages),
            out_shape=jax.ShapeDtypeStruct((chan, tokens), f32),
            in_specs=[vmem, vmem, vmem, hbm, hbm, hbm, hbm, vmem, smem, smem, hbm],
            out_specs=vmem,
            scratch_shapes=[
                pltpu.VMEM((width, 3 * width), bf16),
                pltpu.VMEM((heads, head_dim, width), bf16),
                pltpu.VMEM((width, mlp), bf16),
                pltpu.VMEM((mlp, width), bf16),
                pltpu.VMEM((2, tokens, width), bf16),
                pltpu.VMEM((width, chan), bf16),
                pltpu.VMEM((3 * width, width), bf16),
                pltpu.VMEM((width, width), bf16),
                pltpu.VMEM((mlp, width), bf16),
                pltpu.VMEM((width, mlp), bf16),
                pltpu.VMEM((steps, 128, 128), bf16),
                pltpu.VMEM((3 * width // 128, 128, 256), bf16),
                pltpu.VMEM((6, width, 128), f32),
                pltpu.VMEM((steps, width, tokens), bf16),
                pltpu.VMEM((steps, width, tokens), bf16),
                pltpu.VMEM((steps, chan, tokens), f32),
                pltpu.VMEM((chan, tokens), f32),
                pltpu.VMEM((width, tokens), f32),
                pltpu.VMEM((width, tokens), f32),
                pltpu.VMEM((width, tokens), bf16),
                pltpu.VMEM((width, tokens), bf16),
                pltpu.SemaphoreType.DMA((5,)),
                pltpu.SemaphoreType.DMA((steps,)),
                pltpu.SemaphoreType.DMA((steps,)),
                pltpu.SemaphoreType.DMA((steps,)),
                pltpu.SemaphoreType.DMA((steps,)),
                pltpu.SemaphoreType.DMA((stages,)),
                pltpu.SemaphoreType.DMA,
            ],
            compiler_params=pltpu.CompilerParams(collective_id=0, has_side_effects=True, vmem_limit_bytes=56 * 1024 * 1024),
            name='stage_loop',
        )(jnp.swapaxes(x_init, 1, 2)[0], w_in, jnp.swapaxes(w_out, 0, 1), w_qkv[0], w_proj[0], w_up[0], w_down[0],
          mod_table.reshape(steps * mod_rows, 128), coef_keep, coef_noise, h_warm)
        return jnp.swapaxes(out, 0, 1)[None]

    return jax.shard_map(
        shard_body,
        mesh=mesh,
        in_specs=(P('data'), P(), P(), P('stage'), P('stage'), P('stage'), P('stage'), P(None, 'stage'), P(), P(), P(None, None, 'data')),
        out_specs=P('data'),
        check_vma=False,
    )
```

```python
import functools
import math

import jax
import jax.numpy as jnp
from jax import lax
from jax.experimental import pallas as pl
from jax.experimental.pallas import tpu as pltpu
from jax.sharding import PartitionSpec as P

LN_EPS = 1e-6
LOG2E = math.log2(math.e)
GELU_A = math.sqrt(2.0 / math.pi)
GELU_B = GELU_A * 0.044715
UNIT = 64
MESH = pl.DeviceIdType.MESH


def fold(rows):
    while rows.shape[0] % 16 == 0:
        half = rows.shape[0] // 2
        rows = rows[:half] + rows[half:]
    parts = [rows[lo:lo + 8] for lo in range(0, rows.shape[0], 8)]
    while len(parts) > 1:
        parts = [a + b for a, b in zip(parts[::2], parts[1::2])] + parts[len(parts) - len(parts) % 2:]
    return jnp.sum(parts[0], axis=0, keepdims=True)


def normalize(hidden):
    scale = 1.0 / hidden.shape[0]
    centered = hidden - fold(hidden) * scale
    var = fold(centered * centered) * scale
    return centered * lax.rsqrt(var + LN_EPS)


def dot(lhs, rhs):
    return jnp.dot(lhs, rhs, preferred_element_type=jnp.float32)


def kernel(stages, x_hbm, w_in_hbm, w_out_hbm, qkv_hbm, proj_hbm, up_hbm, down_hbm, mod_hbm, keep_ref, noise_ref, warm_hbm,
           out_ref, x_ref, w_in_ref, w_out_ref, mod_ref, qkv_n, proj_n, up_n, down_n, warm_n, w_in_t, qkv_w, proj_w, up_w, down_w, mod_s, select, lanes,
           recv, sent, x_recv, x_cur, h_last, h_scr, u_scr, o_scr, p_scr, load_sem, recv_sem, send_sem, x_recv_sem, x_send_sem, last_send_sem, last_recv_sem):
    stage = lax.axis_index('stage')
    is_first = stage == 0
    is_last = stage == stages - 1
    steps = keep_ref.shape[0]
    width, tokens = h_last.shape
    heads, head_dim = proj_hbm.shape[0], proj_hbm.shape[1]
    mlp = up_w.shape[0]
    bf16, f32 = jnp.bfloat16, jnp.float32

    loads = [
        pltpu.make_async_copy(warm_hbm.at[:, jnp.maximum(stage - 1, 0), 0], warm_n, load_sem.at[0]),
        pltpu.make_async_copy(qkv_hbm, qkv_n, load_sem.at[1]),
        pltpu.make_async_copy(proj_hbm, proj_n, load_sem.at[2]),
        pltpu.make_async_copy(up_hbm, up_n, load_sem.at[3]),
        pltpu.make_async_copy(down_hbm, down_n, load_sem.at[4]),
        pltpu.make_async_copy(x_hbm, x_ref, load_sem.at[5]),
        pltpu.make_async_copy(w_in_hbm, w_in_ref, load_sem.at[6]),
        pltpu.make_async_copy(w_out_hbm, w_out_ref, load_sem.at[7]),
        pltpu.make_async_copy(mod_hbm, mod_ref, load_sem.at[8]),
    ]
    for index in (8, 5, 6, 7, 0, 1, 2, 3, 4):
        loads[index].start()
    barrier = pltpu.get_barrier_semaphore()
    for ahead in range(1, stages):
        pl.semaphore_signal(barrier, inc=1, device_id={'stage': lax.rem(stage + ahead, stages)}, device_id_type=MESH)

    loads[8].wait()
    mod_rows = mod_ref.shape[0] // steps
    parts = width // 128
    pad = mod_rows + -mod_rows % 8
    row_id = lax.broadcasted_iota(jnp.int32, (mod_rows, 128), 0) // parts
    plus = jnp.where((row_id == 1) | (row_id == 4), 1.0, 0.0)
    limit = float(jnp.finfo(bf16).max)
    gap = jnp.zeros((pad - mod_rows, 128), f32)
    rest_rows = jnp.zeros((128 - 3 * pad, 128), f32)

    for step in range(steps):
        rows = mod_ref[step * mod_rows:(step + 1) * mod_rows] + plus
        high = jnp.clip(rows, -limit, limit).astype(bf16).astype(f32)
        rest = rows - high
        mid = rest.astype(bf16).astype(f32)
        terms = jnp.concatenate([high, gap, mid, gap, rest - mid, gap, rest_rows], axis=0)
        mod_s[step] = terms.T.astype(bf16)

    term = lax.broadcasted_iota(jnp.int32, (128, 256), 0)
    term = jnp.where(term < 3 * pad, term % pad, -1)
    column = lax.broadcasted_iota(jnp.int32, (128, 256), 1) // 128
    for pair in range(3):
        for part in range(parts):
            pick = term == (2 * pair + column) * parts + part
            select[pair * parts + part] = jnp.where(pick, 1.0, 0.0).astype(bf16)

    def fill(step, pair, part):
        return dot(mod_s[step], select[pair * parts + part])

    def store_fill(pair, part, both):
        for side in range(2):
            lanes[2 * pair + side, part * 128:part * 128 + 128] = both[:, side * 128:side * 128 + 128]

    halves = [slice(lo, lo + 128) for lo in range(0, tokens, 128)]

    for index in (5, 6, 7):
        loads[index].wait()
    w_in_t[...] = w_in_ref[...].T
    x_cur[...] = x_ref[...]
    for slot in range(2):
        x_recv[slot] = x_ref[...]
    loads[0].wait()
    for slot in range(2):
        recv[slot] = warm_n[slot].T
    loads[1].wait()
    qkv_w[...] = qkv_n[...].T
    loads[2].wait()
    proj_w[...] = proj_n[...].reshape(width, width).T
    loads[3].wait()
    up_w[...] = up_n[...].T * jnp.asarray(0.5, bf16)
    loads[4].wait()
    down_w[...] = down_n[...].T
    for part in range(parts):
        store_fill(0, part, fill(0, 0, part))
    pl.semaphore_wait(barrier, stages - 1)

    next_id = {'stage': lax.rem(stage + 1, stages)}

    def hidden_copy(step):
        return pltpu.make_async_remote_copy(
            src_ref=sent.at[step], dst_ref=recv.at[step + 2], send_sem=send_sem.at[step], recv_sem=recv_sem.at[step + 2],
            device_id=next_id, device_id_type=MESH)

    def latent_copy(step):
        return pltpu.make_async_remote_copy(
            src_ref=x_recv.at[step + 2], dst_ref=x_recv.at[step + 2], send_sem=x_send_sem.at[step], recv_sem=x_recv_sem.at[step + 2],
            device_id=next_id, device_id_type=MESH)

    first_trips = steps - 2 * (stages - 1)
    trips = first_trips + 2 * stage

    row_units = [slice(lo, lo + UNIT) for lo in range(0, width, UNIT)]

    def to_tile(rows):
        while rows.shape[0] > 8:
            mid = rows.shape[0] // 2
            rows = rows[:mid] + rows[mid:]
        return rows

    def mean_of(tiles_of_half):
        total = tiles_of_half[0::2]
        total = [a + b for a, b in zip(total, tiles_of_half[1::2])]
        while len(total) > 1:
            total = [a + b for a, b in zip(total[::2], total[1::2])] + total[len(total) - len(total) % 2:]
        return jnp.sum(total[0], axis=0, keepdims=True) * (1.0 / width)

    def norm_store(sums, scale_row, shift_row):
        stats = []
        for half, tiles_of_half in zip(halves, sums):
            mean = mean_of(tiles_of_half)
            squares = []
            for rows in row_units:
                centered = h_scr[rows, half] - mean
                squares.append(to_tile(centered * centered))
            stats.append((mean, lax.rsqrt(mean_of(squares) + LN_EPS)))
        for rows in row_units:
            for half, (mean, rstd) in zip(halves, stats):
                u_scr[rows, half] = ((h_scr[rows, half] - mean) * rstd * lanes[scale_row, rows] + lanes[shift_row, rows]).astype(bf16)

    quarter = width // 2
    each = quarter // UNIT

    row_units = [slice(lo, lo + UNIT) for lo in range(0, width, UNIT)]

    def to_tile(rows):
        while rows.shape[0] > 8:
            mid = rows.shape[0] // 2
            rows = rows[:mid] + rows[mid:]
        return rows

    def mean_of(tiles_of_half):
        total = tiles_of_half[0::2]
        total = [a + b for a, b in zip(total, tiles_of_half[1::2])]
        while len(total) > 1:
            total = [a + b for a, b in zip(total[::2], total[1::2])] + total[len(total) - len(total) % 2:]
        return jnp.sum(total[0], axis=0, keepdims=True) * (1.0 / width)

    def norm_store(sums, scale_row, shift_row):
        stats = []
        for half, tiles_of_half in zip(halves, sums):
            mean = mean_of(tiles_of_half)
            squares = []
            for rows in row_units:
                centered = h_scr[rows, half] - mean
                squares.append(to_tile(centered * centered))
            stats.append((mean, lax.rsqrt(mean_of(squares) + LN_EPS)))
        for rows in row_units:
            for half, (mean, rstd) in zip(halves, stats):
                u_scr[rows, half] = ((h_scr[rows, half] - mean) * rstd * lanes[scale_row, rows] + lanes[shift_row, rows]).astype(bf16)

    quarter = width // 2
    each = quarter // UNIT

    def tiles(rows):
        return rows[:256], jnp.concatenate([zeros_half, rows[256:]], axis=0)

    def weight(ref, row, register):
        lo = 0 if register == 0 else width - 256
        return ref[row:row + UNIT, lo:lo + 256]

    def block(step, hidden_in, beside=lambda: None):
        fills = {(pair, part): fill(step, pair, part) for pair in (1, 2) for part in range(parts)}
        sums = [[], []]
        for rows in row_units:
            for side, half in enumerate(halves):
                hidden = hidden_in(half, rows)
                h_scr[rows, half] = hidden
                sums[side].append(to_tile(hidden))
        norm_store(sums, 1, 0)
        normed = u_scr[...]
        pairs = heads // 2

        def project_in(kind, lo, hi):
            start = kind * width
            return dot(qkv_w[start + lo * head_dim:start + hi * head_dim], normed).astype(bf16)

        def per_head(rows):
            return [rows[lo:lo + head_dim] for lo in range(0, rows.shape[0], head_dim)]

        groups = ((0, 2), (2, heads))
        keys, queries = [], []
        for lo, hi in groups:
            keys += per_head(project_in(1, lo, hi))
            queries += per_head(project_in(0, lo, hi))
        for (pair, part), both in fills.items():
            store_fill(pair, part, both)
        factor = LOG2E * head_dim ** -0.5

        def score(index):
            return [dot(keys[head].T, queries[head]) for head in (2 * index, 2 * index + 1)]

        def softmax(scores):
            top = jnp.max(scores, axis=0, keepdims=True)
            expo = jnp.exp2((scores - top) * factor)
            return expo.astype(bf16), 1.0 / fold(expo)

        scores = [score(0)]
        values = per_head(project_in(2, 0, heads // 2)) + per_head(project_in(2, heads // 2, heads))
        beside()
        proj = [None, None]

        def project_out(lo, hi):
            for side in range(2):
                piece = dot(proj_w[side * quarter:side * quarter + quarter, lo:hi], o_scr[lo:hi])
                if lo == 0:
                    p_scr[side * quarter:side * quarter + quarter] = piece
                else:
                    proj[side] = piece

        for index in range(pairs):
            if index + 1 < pairs:
                scores.append(score(index + 1))
            outs = []
            for unit in range(2):
                head = 2 * index + unit
                done = [softmax(scores[index][unit][:, half]) for half in halves]
                inverse = jnp.concatenate([pair[1] for pair in done], axis=1)
                expo = jnp.concatenate([pair[0] for pair in done], axis=1)
                outs.append((dot(values[head], expo), inverse))
            if index == pairs - 1:
                project_out(0, 256)
            for unit, (out, inverse) in enumerate(outs):
                head = 2 * index + unit
                o_scr[head * head_dim:(head + 1) * head_dim] = (out * inverse).astype(bf16)
        project_out(256, width)
        sums = [[], []]
        for unit in range(2):
            for part in range(each):
                lo = unit * quarter + part * UNIT
                rows = slice(lo, lo + UNIT)
                piece = proj[unit][part * UNIT:part * UNIT + UNIT] + p_scr[rows]
                for side, half in enumerate(halves):
                    hidden = h_scr[rows, half] + lanes[2, rows] * piece[:, half]
                    h_scr[rows, half] = hidden
                    sums[side].append(to_tile(hidden))
        norm_store(sums, 4, 3)
        normed = u_scr[...]
        tile_count = mlp // 256
        ups = [dot(up_w[tile * 256:tile * 256 + 256], normed) for tile in range(tile_count)]

        def gelu(pre):
            return (pre * jnp.tanh(pre * (2.0 * GELU_A + 8.0 * GELU_B * (pre * pre))) + pre).astype(bf16)

        after = jnp.minimum(step + 1, steps - 1)
        down = [None, None]
        for tile in range(tile_count):
            act = jnp.concatenate([gelu(ups[tile][lo:lo + UNIT]) for lo in range(0, 256, UNIT)], axis=0)
            if tile == tile_count - 1:
                for part in range(parts):
                    store_fill(0, part, fill(after, 0, part))
            for side in range(2):
                piece = dot(down_w[side * quarter:side * quarter + quarter, tile * 256:tile * 256 + 256], act)
                down[side] = piece if down[side] is None else down[side] + piece
        for unit in range(2):
            for part in range(each):
                lo = unit * quarter + part * UNIT
                rows = slice(lo, lo + UNIT)
                for half in halves:
                    yield rows, half, h_scr[rows, half] + lanes[5, rows] * down[unit][part * UNIT:part * UNIT + UNIT, half]

    def send(step, columns):
        for rows, half, hidden in columns:
            sent[step, rows, half] = hidden.astype(bf16)
        hidden_copy(step).start()

    def received(step):
        return lambda half, rows=slice(None): recv[step, rows, half].astype(f32)

    def wait_hidden(step):
        @pl.when(step >= 2)
        def _():
            hidden_copy(step - 2).wait_recv()

    def first_step(step, carry):
        @pl.when(step >= 2)
        def _():
            latent_copy(step - 2).wait_recv()
        h_last[...] = dot(w_in_t[...], x_recv[step].astype(bf16))
        send(step, block(step, lambda half, rows=slice(None): h_last[rows, half]))
        return carry

    def middle_step(step, carry):
        wait_hidden(step)
        send(step, block(step, received(step)))
        return carry

    def advance(step):
        normed = jnp.concatenate([normalize(h_last[:, half]).astype(bf16) for half in halves], axis=1)
        noise = dot(w_out_ref[...], normed)
        x_next = keep_ref[step] * x_cur[...] + noise_ref[step] * noise
        x_cur[...] = x_next
        return x_next

    def last_step(step, carry):
        wait_hidden(step)
        before = jnp.maximum(step - 1, 0)

        def beside():
            x_next = jnp.where(step > 0, advance(before), x_ref[...])
            x_cur[...] = x_next
            x_recv[jnp.minimum(before + 2, steps - 1)] = x_next

        for rows, half, hidden in block(step, received(step), beside):
            h_last[rows, half] = hidden

        @pl.when((step > 0) & (before + 2 < first_trips))
        def _():
            latent_copy(before).start()
        return carry

    def final_copy(ahead):
        return pltpu.make_async_remote_copy(
            src_ref=x_cur, dst_ref=out_ref, send_sem=last_send_sem.at[ahead], recv_sem=last_recv_sem,
            device_id={'stage': lax.rem(stage + ahead, stages)}, device_id_type=MESH)

    @pl.when(is_first)
    def _():
        lax.fori_loop(0, first_trips, first_step, 0)

    @pl.when(jnp.logical_not(is_first | is_last))
    def _():
        lax.fori_loop(0, trips, middle_step, 0)

    @pl.when(is_last)
    def _():
        h_last[...] = jnp.zeros_like(h_last)
        lax.fori_loop(0, steps, last_step, 0)
        out_ref[...] = advance(steps - 1)
        for ahead in range(1, stages):
            final_copy(ahead).start()
        for ahead in range(1, stages):
            final_copy(ahead).wait_send()

        def drain(step, carry):
            latent_copy(step).wait_send()
            return carry
        lax.fori_loop(0, first_trips - 2, drain, 0)

    @pl.when(jnp.logical_not(is_last))
    def _():
        def drain(step, carry):
            hidden_copy(step).wait_send()
            return carry
        lax.fori_loop(0, trips, drain, 0)
        final_copy(1).wait_recv()


def solution(mesh):
    stages = mesh.shape['stage']

    def shard_body(x_init, w_in, w_out, w_qkv, w_proj, w_up, w_down, mod_table, coef_keep, coef_noise, h_warm):
        steps = coef_keep.shape[0]
        tokens, chan = x_init.shape[1], x_init.shape[2]
        width, mlp = w_up.shape[1], w_up.shape[2]
        heads, head_dim = w_proj.shape[1], w_proj.shape[2]
        mod_rows = mod_table.shape[2] * width // 128
        bf16, f32 = jnp.bfloat16, jnp.float32
        vmem = pl.BlockSpec(memory_space=pltpu.VMEM)
        smem = pl.BlockSpec(memory_space=pltpu.SMEM)
        hbm = pl.BlockSpec(memory_space=pl.ANY)
        out = pl.pallas_call(
            functools.partial(kernel, stages),
            out_shape=jax.ShapeDtypeStruct((chan, tokens), f32),
            in_specs=[hbm] * 8 + [smem, smem, hbm],
            out_specs=vmem,
            scratch_shapes=[
                pltpu.VMEM((chan, tokens), f32),
                pltpu.VMEM((chan, width), bf16),
                pltpu.VMEM((chan, width), bf16),
                pltpu.VMEM((steps * mod_rows, 128), f32),
                pltpu.VMEM((width, 3 * width), bf16),
                pltpu.VMEM((heads, head_dim, width), bf16),
                pltpu.VMEM((width, mlp), bf16),
                pltpu.VMEM((mlp, width), bf16),
                pltpu.VMEM((2, tokens, width), bf16),
                pltpu.VMEM((width, chan), bf16),
                pltpu.VMEM((3 * width, width), bf16),
                pltpu.VMEM((width, width), bf16),
                pltpu.VMEM((mlp, width), bf16),
                pltpu.VMEM((width, mlp), bf16),
                pltpu.VMEM((steps, 128, 128), bf16),
                pltpu.VMEM((3 * width // 128, 128, 256), bf16),
                pltpu.VMEM((6, width, 128), f32),
                pltpu.VMEM((steps, width, tokens), bf16),
                pltpu.VMEM((steps, width, tokens), bf16),
                pltpu.VMEM((steps, chan, tokens), f32),
                pltpu.VMEM((chan, tokens), f32),
                pltpu.VMEM((width, tokens), f32),
                pltpu.VMEM((width, tokens), f32),
                pltpu.VMEM((width, tokens), bf16),
                pltpu.VMEM((width, tokens), bf16),
                pltpu.VMEM((width, tokens), f32),
                pltpu.SemaphoreType.DMA((9,)),
                pltpu.SemaphoreType.DMA((steps,)),
                pltpu.SemaphoreType.DMA((steps,)),
                pltpu.SemaphoreType.DMA((steps,)),
                pltpu.SemaphoreType.DMA((steps,)),
                pltpu.SemaphoreType.DMA((stages,)),
                pltpu.SemaphoreType.DMA,
            ],
            compiler_params=pltpu.CompilerParams(collective_id=0, has_side_effects=True, vmem_limit_bytes=56 * 1024 * 1024),
            name='stage_loop',
        )(jnp.swapaxes(x_init, 1, 2)[0], w_in, jnp.swapaxes(w_out, 0, 1), w_qkv[0], w_proj[0], w_up[0], w_down[0],
          mod_table.reshape(steps * mod_rows, 128), coef_keep, coef_noise, h_warm)
        return jnp.swapaxes(out, 0, 1)[None]

    return jax.shard_map(
        shard_body,
        mesh=mesh,
        in_specs=(P('data'), P(), P(), P('stage'), P('stage'), P('stage'), P('stage'), P(None, 'stage'), P(), P(), P(None, None, 'data')),
        out_specs=P('data'),
        check_vma=False,
    )
```

```python
import functools
import math

import jax
import jax.numpy as jnp
from jax import lax
from jax.experimental import pallas as pl
from jax.experimental.pallas import tpu as pltpu
from jax.sharding import PartitionSpec as P

LN_EPS = 1e-6
LOG2E = math.log2(math.e)
GELU_A = math.sqrt(2.0 / math.pi)
GELU_B = GELU_A * 0.044715
UNIT = 64
MESH = pl.DeviceIdType.MESH


def fold(rows):
    while rows.shape[0] % 16 == 0:
        half = rows.shape[0] // 2
        rows = rows[:half] + rows[half:]
    parts = [rows[lo:lo + 8] for lo in range(0, rows.shape[0], 8)]
    while len(parts) > 1:
        parts = [a + b for a, b in zip(parts[::2], parts[1::2])] + parts[len(parts) - len(parts) % 2:]
    return jnp.sum(parts[0], axis=0, keepdims=True)


def normalize(hidden):
    scale = 1.0 / hidden.shape[0]
    centered = hidden - fold(hidden) * scale
    var = fold(centered * centered) * scale
    return centered * lax.rsqrt(var + LN_EPS)


def dot(lhs, rhs):
    return jnp.dot(lhs, rhs, preferred_element_type=jnp.float32)


def kernel(stages, x_hbm, w_in_hbm, w_out_hbm, qkv_hbm, proj_hbm, up_hbm, down_hbm, mod_hbm, keep_ref, noise_ref, warm_hbm,
           out_ref, x_ref, w_in_ref, w_out_ref, mod_ref, qkv_n, proj_n, up_n, down_n, warm_n, w_in_t, qkv_w, proj_w, up_w, down_w, mod_s, select, lanes,
           recv, sent, x_recv, x_cur, h_last, h_scr, u_scr, o_scr, p_scr, load_sem, recv_sem, send_sem, x_recv_sem, x_send_sem, last_send_sem, last_recv_sem):
    stage = lax.axis_index('stage')
    is_first = stage == 0
    is_last = stage == stages - 1
    steps = keep_ref.shape[0]
    width, tokens = h_last.shape
    heads, head_dim = proj_hbm.shape[0], proj_hbm.shape[1]
    mlp = up_w.shape[0]
    bf16, f32 = jnp.bfloat16, jnp.float32

    loads = [
        pltpu.make_async_copy(warm_hbm.at[:, jnp.maximum(stage - 1, 0), 0], warm_n, load_sem.at[0]),
        pltpu.make_async_copy(qkv_hbm, qkv_n, load_sem.at[1]),
        pltpu.make_async_copy(proj_hbm, proj_n, load_sem.at[2]),
        pltpu.make_async_copy(up_hbm, up_n, load_sem.at[3]),
        pltpu.make_async_copy(down_hbm, down_n, load_sem.at[4]),
        pltpu.make_async_copy(x_hbm, x_ref, load_sem.at[5]),
        pltpu.make_async_copy(w_in_hbm, w_in_ref, load_sem.at[6]),
        pltpu.make_async_copy(w_out_hbm, w_out_ref, load_sem.at[7]),
        pltpu.make_async_copy(mod_hbm, mod_ref, load_sem.at[8]),
    ]
    for index in (8, 5, 6, 7, 0, 1, 2, 3, 4):
        loads[index].start()
    barrier = pltpu.get_barrier_semaphore()
    for ahead in range(1, stages):
        pl.semaphore_signal(barrier, inc=1, device_id={'stage': lax.rem(stage + ahead, stages)}, device_id_type=MESH)

    loads[8].wait()
    mod_rows = mod_ref.shape[0] // steps
    parts = width // 128
    pad = mod_rows + -mod_rows % 8
    row_id = lax.broadcasted_iota(jnp.int32, (mod_rows, 128), 0) // parts
    plus = jnp.where((row_id == 1) | (row_id == 4), 1.0, 0.0)
    limit = float(jnp.finfo(bf16).max)
    gap = jnp.zeros((pad - mod_rows, 128), f32)
    rest_rows = jnp.zeros((128 - 3 * pad, 128), f32)

    for step in range(steps):
        rows = mod_ref[step * mod_rows:(step + 1) * mod_rows] + plus
        high = jnp.clip(rows, -limit, limit).astype(bf16).astype(f32)
        rest = rows - high
        mid = rest.astype(bf16).astype(f32)
        terms = jnp.concatenate([high, gap, mid, gap, rest - mid, gap, rest_rows], axis=0)
        mod_s[step] = terms.T.astype(bf16)

    term = lax.broadcasted_iota(jnp.int32, (128, 256), 0)
    term = jnp.where(term < 3 * pad, term % pad, -1)
    column = lax.broadcasted_iota(jnp.int32, (128, 256), 1) // 128
    for pair in range(3):
        for part in range(parts):
            pick = term == (2 * pair + column) * parts + part
            select[pair * parts + part] = jnp.where(pick, 1.0, 0.0).astype(bf16)

    def fill(step, pair, part):
        return dot(mod_s[step], select[pair * parts + part])

    def store_fill(pair, part, both):
        for side in range(2):
            lanes[2 * pair + side, part * 128:part * 128 + 128] = both[:, side * 128:side * 128 + 128]

    halves = [slice(lo, lo + 128) for lo in range(0, tokens, 128)]

    for index in (5, 6, 7):
        loads[index].wait()
    w_in_t[...] = w_in_ref[...].T
    x_cur[...] = x_ref[...]
    for slot in range(2):
        x_recv[slot] = x_ref[...]
    loads[0].wait()
    for slot in range(2):
        recv[slot] = warm_n[slot].T
    loads[1].wait()
    qkv_w[...] = qkv_n[...].T
    loads[2].wait()
    proj_w[...] = proj_n[...].reshape(width, width).T
    loads[3].wait()
    up_w[...] = up_n[...].T * jnp.asarray(0.5, bf16)
    loads[4].wait()
    down_w[...] = down_n[...].T
    for part in range(parts):
        store_fill(0, part, fill(0, 0, part))
    pl.semaphore_wait(barrier, stages - 1)

    next_id = {'stage': lax.rem(stage + 1, stages)}

    def hidden_copy(step):
        return pltpu.make_async_remote_copy(
            src_ref=sent.at[step], dst_ref=recv.at[step + 2], send_sem=send_sem.at[step], recv_sem=recv_sem.at[step + 2],
            device_id=next_id, device_id_type=MESH)

    def latent_copy(step):
        return pltpu.make_async_remote_copy(
            src_ref=x_recv.at[step + 2], dst_ref=x_recv.at[step + 2], send_sem=x_send_sem.at[step], recv_sem=x_recv_sem.at[step + 2],
            device_id=next_id, device_id_type=MESH)

    first_trips = steps - 2 * (stages - 1)
    trips = first_trips + 2 * stage

    row_units = [slice(lo, lo + UNIT) for lo in range(0, width, UNIT)]

    def to_tile(rows):
        while rows.shape[0] > 8:
            mid = rows.shape[0] // 2
            rows = rows[:mid] + rows[mid:]
        return rows

    def mean_of(tiles_of_half):
        total = tiles_of_half[0::2]
        total = [a + b for a, b in zip(total, tiles_of_half[1::2])]
        while len(total) > 1:
            total = [a + b for a, b in zip(total[::2], total[1::2])] + total[len(total) - len(total) % 2:]
        return jnp.sum(total[0], axis=0, keepdims=True) * (1.0 / width)

    def norm_store(sums, scale_row, shift_row):
        stats = []
        for half, tiles_of_half in zip(halves, sums):
            mean = mean_of(tiles_of_half)
            squares = []
            for rows in row_units:
                centered = h_scr[rows, half] - mean
                squares.append(to_tile(centered * centered))
            stats.append((mean, lax.rsqrt(mean_of(squares) + LN_EPS)))
        for rows in row_units:
            for half, (mean, rstd) in zip(halves, stats):
                u_scr[rows, half] = ((h_scr[rows, half] - mean) * rstd * lanes[scale_row, rows] + lanes[shift_row, rows]).astype(bf16)

    quarter = width // 2
    each = quarter // UNIT

    row_units = [slice(lo, lo + UNIT) for lo in range(0, width, UNIT)]

    def to_tile(rows):
        while rows.shape[0] > 8:
            mid = rows.shape[0] // 2
            rows = rows[:mid] + rows[mid:]
        return rows

    def mean_of(tiles_of_half):
        total = tiles_of_half[0::2]
        total = [a + b for a, b in zip(total, tiles_of_half[1::2])]
        while len(total) > 1:
            total = [a + b for a, b in zip(total[::2], total[1::2])] + total[len(total) - len(total) % 2:]
        return jnp.sum(total[0], axis=0, keepdims=True) * (1.0 / width)

    def norm_store(sums, scale_row, shift_row):
        stats = []
        for half, tiles_of_half in zip(halves, sums):
            mean = mean_of(tiles_of_half)
            squares = []
            for rows in row_units:
                centered = h_scr[rows, half] - mean
                squares.append(to_tile(centered * centered))
            stats.append((mean, lax.rsqrt(mean_of(squares) + LN_EPS)))
        for rows in row_units:
            for half, (mean, rstd) in zip(halves, stats):
                u_scr[rows, half] = ((h_scr[rows, half] - mean) * rstd * lanes[scale_row, rows] + lanes[shift_row, rows]).astype(bf16)

    quarter = width // 2
    each = quarter // UNIT

    def tiles(rows):
        return rows[:256], jnp.concatenate([zeros_half, rows[256:]], axis=0)

    def weight(ref, row, register):
        lo = 0 if register == 0 else width - 256
        return ref[row:row + UNIT, lo:lo + 256]

    def block(step, hidden_in, beside=lambda: None):
        fills = {(pair, part): fill(step, pair, part) for pair in (1, 2) for part in range(parts)}
        sums = [[], []]
        for rows in row_units:
            for side, half in enumerate(halves):
                hidden = hidden_in(half, rows)
                h_scr[rows, half] = hidden
                sums[side].append(to_tile(hidden))
        norm_store(sums, 1, 0)
        normed = u_scr[...]
        pairs = heads // 2

        def project_in(kind, lo, hi):
            start = kind * width
            return dot(qkv_w[start + lo * head_dim:start + hi * head_dim], normed).astype(bf16)

        def per_head(rows):
            return [rows[lo:lo + head_dim] for lo in range(0, rows.shape[0], head_dim)]

        groups = ((0, 2), (2, heads))
        keys, queries = [], []
        for lo, hi in groups:
            keys += per_head(project_in(1, lo, hi))
            queries += per_head(project_in(0, lo, hi))
        for (pair, part), both in fills.items():
            store_fill(pair, part, both)
        factor = LOG2E * head_dim ** -0.5

        def score(index):
            return [dot(keys[head].T, queries[head]) for head in (2 * index, 2 * index + 1)]

        def softmax(scores):
            top = jnp.max(scores, axis=0, keepdims=True)
            expo = jnp.exp2((scores - top) * factor)
            return expo.astype(bf16), 1.0 / fold(expo)

        beside()
        scores = [score(0)]
        values = per_head(project_in(2, 0, 2))
        scores.append(score(1))
        values += per_head(project_in(2, 2, heads))
        proj = [None, None]

        def project_out(lo, hi):
            for side in range(2):
                piece = dot(proj_w[side * quarter:side * quarter + quarter, lo:hi], o_scr[lo:hi])
                if lo == 0:
                    p_scr[side * quarter:side * quarter + quarter] = piece
                else:
                    proj[side] = piece

        for index in range(pairs):
            if index + 2 < pairs:
                scores.append(score(index + 2))
            outs = []
            for unit in range(2):
                head = 2 * index + unit
                done = [softmax(scores[index][unit][:, half]) for half in halves]
                inverse = jnp.concatenate([pair[1] for pair in done], axis=1)
                expo = jnp.concatenate([pair[0] for pair in done], axis=1)
                outs.append((dot(values[head], expo), inverse))
            if index == pairs - 1:
                project_out(0, 256)
                after = jnp.minimum(step + 1, steps - 1)
                for part in range(parts):
                    store_fill(0, part, fill(after, 0, part))
            for unit, (out, inverse) in enumerate(outs):
                head = 2 * index + unit
                o_scr[head * head_dim:(head + 1) * head_dim] = (out * inverse).astype(bf16)
        project_out(256, width)
        sums = [[], []]
        for unit in range(2):
            for part in range(each):
                lo = unit * quarter + part * UNIT
                rows = slice(lo, lo + UNIT)
                piece = proj[unit][part * UNIT:part * UNIT + UNIT] + p_scr[rows]
                for side, half in enumerate(halves):
                    hidden = h_scr[rows, half] + lanes[2, rows] * piece[:, half]
                    h_scr[rows, half] = hidden
                    sums[side].append(to_tile(hidden))
        norm_store(sums, 4, 3)
        normed = u_scr[...]
        tile_count = mlp // 256
        ups = [dot(up_w[tile * 256:tile * 256 + 256], normed) for tile in range(tile_count)]

        def gelu(pre):
            return (pre * jnp.tanh(pre * (2.0 * GELU_A + 8.0 * GELU_B * (pre * pre))) + pre).astype(bf16)

        down = [None, None]
        for tile in range(tile_count):
            act = jnp.concatenate([gelu(ups[tile][lo:lo + UNIT]) for lo in range(0, 256, UNIT)], axis=0)
            for side in range(2):
                piece = dot(down_w[side * quarter:side * quarter + quarter, tile * 256:tile * 256 + 256], act)
                down[side] = piece if down[side] is None else down[side] + piece
        for unit in range(2):
            for part in range(each):
                lo = unit * quarter + part * UNIT
                rows = slice(lo, lo + UNIT)
                for half in halves:
                    yield rows, half, h_scr[rows, half] + lanes[5, rows] * down[unit][part * UNIT:part * UNIT + UNIT, half]

    def send(step, columns):
        for rows, half, hidden in columns:
            sent[step, rows, half] = hidden.astype(bf16)
        hidden_copy(step).start()

    def received(step):
        return lambda half, rows=slice(None): recv[step, rows, half].astype(f32)

    def wait_hidden(step):
        @pl.when(step >= 2)
        def _():
            hidden_copy(step - 2).wait_recv()

    def first_step(step, carry):
        @pl.when(step >= 2)
        def _():
            latent_copy(step - 2).wait_recv()
        h_last[...] = dot(w_in_t[...], x_recv[step].astype(bf16))
        send(step, block(step, lambda half, rows=slice(None): h_last[rows, half]))
        return carry

    def middle_step(step, carry):
        wait_hidden(step)
        send(step, block(step, received(step)))
        return carry

    def advance(step):
        normed = jnp.concatenate([normalize(h_last[:, half]).astype(bf16) for half in halves], axis=1)
        noise = dot(w_out_ref[...], normed)
        x_next = keep_ref[step] * x_cur[...] + noise_ref[step] * noise
        x_cur[...] = x_next
        return x_next

    def last_step(step, carry):
        wait_hidden(step)
        before = jnp.maximum(step - 1, 0)

        def beside():
            x_next = jnp.where(step > 0, advance(before), x_ref[...])
            x_cur[...] = x_next
            x_recv[jnp.minimum(before + 2, steps - 1)] = x_next

        for rows, half, hidden in block(step, received(step), beside):
            h_last[rows, half] = hidden

        @pl.when((step > 0) & (before + 2 < first_trips))
        def _():
            latent_copy(before).start()
        return carry

    def final_copy(ahead):
        return pltpu.make_async_remote_copy(
            src_ref=x_cur, dst_ref=out_ref, send_sem=last_send_sem.at[ahead], recv_sem=last_recv_sem,
            device_id={'stage': lax.rem(stage + ahead, stages)}, device_id_type=MESH)

    @pl.when(is_first)
    def _():
        lax.fori_loop(0, first_trips, first_step, 0)

    @pl.when(jnp.logical_not(is_first | is_last))
    def _():
        lax.fori_loop(0, trips, middle_step, 0)

    @pl.when(is_last)
    def _():
        h_last[...] = jnp.zeros_like(h_last)
        lax.fori_loop(0, steps, last_step, 0)
        out_ref[...] = advance(steps - 1)
        for ahead in range(1, stages):
            final_copy(ahead).start()
        for ahead in range(1, stages):
            final_copy(ahead).wait_send()

        def drain(step, carry):
            latent_copy(step).wait_send()
            return carry
        lax.fori_loop(0, first_trips - 2, drain, 0)

    @pl.when(jnp.logical_not(is_last))
    def _():
        def drain(step, carry):
            hidden_copy(step).wait_send()
            return carry
        lax.fori_loop(0, trips, drain, 0)
        final_copy(1).wait_recv()


def solution(mesh):
    stages = mesh.shape['stage']

    def shard_body(x_init, w_in, w_out, w_qkv, w_proj, w_up, w_down, mod_table, coef_keep, coef_noise, h_warm):
        steps = coef_keep.shape[0]
        tokens, chan = x_init.shape[1], x_init.shape[2]
        width, mlp = w_up.shape[1], w_up.shape[2]
        heads, head_dim = w_proj.shape[1], w_proj.shape[2]
        mod_rows = mod_table.shape[2] * width // 128
        bf16, f32 = jnp.bfloat16, jnp.float32
        vmem = pl.BlockSpec(memory_space=pltpu.VMEM)
        smem = pl.BlockSpec(memory_space=pltpu.SMEM)
        hbm = pl.BlockSpec(memory_space=pl.ANY)
        out = pl.pallas_call(
            functools.partial(kernel, stages),
            out_shape=jax.ShapeDtypeStruct((chan, tokens), f32),
            in_specs=[hbm] * 8 + [smem, smem, hbm],
            out_specs=vmem,
            scratch_shapes=[
                pltpu.VMEM((chan, tokens), f32),
                pltpu.VMEM((chan, width), bf16),
                pltpu.VMEM((chan, width), bf16),
                pltpu.VMEM((steps * mod_rows, 128), f32),
                pltpu.VMEM((width, 3 * width), bf16),
                pltpu.VMEM((heads, head_dim, width), bf16),
                pltpu.VMEM((width, mlp), bf16),
                pltpu.VMEM((mlp, width), bf16),
                pltpu.VMEM((2, tokens, width), bf16),
                pltpu.VMEM((width, chan), bf16),
                pltpu.VMEM((3 * width, width), bf16),
                pltpu.VMEM((width, width), bf16),
                pltpu.VMEM((mlp, width), bf16),
                pltpu.VMEM((width, mlp), bf16),
                pltpu.VMEM((steps, 128, 128), bf16),
                pltpu.VMEM((3 * width // 128, 128, 256), bf16),
                pltpu.VMEM((6, width, 128), f32),
                pltpu.VMEM((steps, width, tokens), bf16),
                pltpu.VMEM((steps, width, tokens), bf16),
                pltpu.VMEM((steps, chan, tokens), f32),
                pltpu.VMEM((chan, tokens), f32),
                pltpu.VMEM((width, tokens), f32),
                pltpu.VMEM((width, tokens), f32),
                pltpu.VMEM((width, tokens), bf16),
                pltpu.VMEM((width, tokens), bf16),
                pltpu.VMEM((width, tokens), f32),
                pltpu.SemaphoreType.DMA((9,)),
                pltpu.SemaphoreType.DMA((steps,)),
                pltpu.SemaphoreType.DMA((steps,)),
                pltpu.SemaphoreType.DMA((steps,)),
                pltpu.SemaphoreType.DMA((steps,)),
                pltpu.SemaphoreType.DMA((stages,)),
                pltpu.SemaphoreType.DMA,
            ],
            compiler_params=pltpu.CompilerParams(collective_id=0, has_side_effects=True, vmem_limit_bytes=56 * 1024 * 1024),
            name='stage_loop',
        )(jnp.swapaxes(x_init, 1, 2)[0], w_in, jnp.swapaxes(w_out, 0, 1), w_qkv[0], w_proj[0], w_up[0], w_down[0],
          mod_table.reshape(steps * mod_rows, 128), coef_keep, coef_noise, h_warm)
        return jnp.swapaxes(out, 0, 1)[None]

    return jax.shard_map(
        shard_body,
        mesh=mesh,
        in_specs=(P('data'), P(), P(), P('stage'), P('stage'), P('stage'), P('stage'), P(None, 'stage'), P(), P(), P(None, None, 'data')),
        out_specs=P('data'),
        check_vma=False,
    )
```

```python
import functools
import math

import jax
import jax.numpy as jnp
from jax import lax
from jax.experimental import pallas as pl
from jax.experimental.pallas import tpu as pltpu
from jax.sharding import PartitionSpec as P

LN_EPS = 1e-6
LOG2E = math.log2(math.e)
GELU_A = math.sqrt(2.0 / math.pi)
GELU_B = GELU_A * 0.044715
UNIT = 64
MESH = pl.DeviceIdType.MESH


def fold(rows):
    while rows.shape[0] % 16 == 0:
        half = rows.shape[0] // 2
        rows = rows[:half] + rows[half:]
    parts = [rows[lo:lo + 8] for lo in range(0, rows.shape[0], 8)]
    while len(parts) > 1:
        parts = [a + b for a, b in zip(parts[::2], parts[1::2])] + parts[len(parts) - len(parts) % 2:]
    return jnp.sum(parts[0], axis=0, keepdims=True)


def normalize(hidden):
    scale = 1.0 / hidden.shape[0]
    centered = hidden - fold(hidden) * scale
    var = fold(centered * centered) * scale
    return centered * lax.rsqrt(var + LN_EPS)


def dot(lhs, rhs):
    return jnp.dot(lhs, rhs, preferred_element_type=jnp.float32)


def kernel(stages, x_hbm, w_in_hbm, w_out_hbm, qkv_hbm, proj_hbm, up_hbm, down_hbm, mod_hbm, keep_ref, noise_ref, warm_hbm,
           out_ref, x_ref, w_in_ref, w_out_ref, mod_ref, qkv_n, proj_n, up_n, down_n, warm_n, w_in_t, qkv_w, proj_w, up_w, down_w, mod_s, select, lanes,
           recv, sent, x_recv, x_cur, h_last, h_scr, u_scr, o_scr, p_scr, load_sem, recv_sem, send_sem, x_recv_sem, x_send_sem, last_send_sem, last_recv_sem):
    stage = lax.axis_index('stage')
    is_first = stage == 0
    is_last = stage == stages - 1
    steps = keep_ref.shape[0]
    width, tokens = h_last.shape
    heads, head_dim = proj_hbm.shape[0], proj_hbm.shape[1]
    mlp = up_w.shape[0]
    bf16, f32 = jnp.bfloat16, jnp.float32

    loads = [
        pltpu.make_async_copy(warm_hbm.at[:, jnp.maximum(stage - 1, 0), 0], warm_n, load_sem.at[0]),
        pltpu.make_async_copy(qkv_hbm, qkv_n, load_sem.at[1]),
        pltpu.make_async_copy(proj_hbm, proj_n, load_sem.at[2]),
        pltpu.make_async_copy(up_hbm, up_n, load_sem.at[3]),
        pltpu.make_async_copy(down_hbm, down_n, load_sem.at[4]),
        pltpu.make_async_copy(x_hbm, x_ref, load_sem.at[5]),
        pltpu.make_async_copy(w_in_hbm, w_in_ref, load_sem.at[6]),
        pltpu.make_async_copy(w_out_hbm, w_out_ref, load_sem.at[7]),
        pltpu.make_async_copy(mod_hbm, mod_ref, load_sem.at[8]),
    ]
    for index in (8, 5, 6, 7, 0, 1, 2, 3, 4):
        loads[index].start()
    barrier = pltpu.get_barrier_semaphore()
    for ahead in range(1, stages):
        pl.semaphore_signal(barrier, inc=1, device_id={'stage': lax.rem(stage + ahead, stages)}, device_id_type=MESH)

    loads[8].wait()
    mod_rows = mod_ref.shape[0] // steps
    parts = width // 128
    pad = mod_rows + -mod_rows % 8
    row_id = lax.broadcasted_iota(jnp.int32, (mod_rows, 128), 0) // parts
    plus = jnp.where((row_id == 1) | (row_id == 4), 1.0, 0.0)
    limit = float(jnp.finfo(bf16).max)
    gap = jnp.zeros((pad - mod_rows, 128), f32)
    rest_rows = jnp.zeros((128 - 3 * pad, 128), f32)

    for step in range(steps):
        rows = mod_ref[step * mod_rows:(step + 1) * mod_rows] + plus
        high = jnp.clip(rows, -limit, limit).astype(bf16).astype(f32)
        rest = rows - high
        mid = rest.astype(bf16).astype(f32)
        terms = jnp.concatenate([high, gap, mid, gap, rest - mid, gap, rest_rows], axis=0)
        mod_s[step] = terms.T.astype(bf16)

    term = lax.broadcasted_iota(jnp.int32, (128, 256), 0)
    term = jnp.where(term < 3 * pad, term % pad, -1)
    column = lax.broadcasted_iota(jnp.int32, (128, 256), 1) // 128
    for pair in range(3):
        for part in range(parts):
            pick = term == (2 * pair + column) * parts + part
            select[pair * parts + part] = jnp.where(pick, 1.0, 0.0).astype(bf16)

    def fill(step, pair, part):
        return dot(mod_s[step], select[pair * parts + part])

    def store_fill(pair, part, both):
        for side in range(2):
            lanes[2 * pair + side, part * 128:part * 128 + 128] = both[:, side * 128:side * 128 + 128]

    halves = [slice(lo, lo + 128) for lo in range(0, tokens, 128)]

    for index in (5, 6, 7):
        loads[index].wait()
    w_in_t[...] = w_in_ref[...].T
    x_cur[...] = x_ref[...]
    x_recv[0] = x_ref[...]
    for index in range(5):
        loads[index].wait()
    for slot in range(2):
        recv[slot] = warm_n[slot].T
    qkv_w[:2 * width] = qkv_n[:, :2 * width].T
    qkv_w[2 * width:] = qkv_n[:, 2 * width:].T * jnp.asarray(1.0 / tokens, bf16)
    proj_w[...] = proj_n[...].reshape(width, width).T
    up_w[...] = up_n[...].T * jnp.asarray(0.5, bf16)
    down_w[...] = down_n[...].T
    for part in range(parts):
        store_fill(0, part, fill(0, 0, part))
    pl.semaphore_wait(barrier, stages - 1)

    next_id = {'stage': lax.rem(stage + 1, stages)}

    def hidden_copy(step):
        return pltpu.make_async_remote_copy(
            src_ref=sent.at[step], dst_ref=recv.at[step + 2], send_sem=send_sem.at[step], recv_sem=recv_sem.at[step + 2],
            device_id=next_id, device_id_type=MESH)

    def latent_copy(step):
        return pltpu.make_async_remote_copy(
            src_ref=x_recv.at[step + 1], dst_ref=x_recv.at[step + 1], send_sem=x_send_sem.at[step], recv_sem=x_recv_sem.at[step],
            device_id=next_id, device_id_type=MESH)

    first_trips = steps - 2 * (stages - 1)
    trips = first_trips + 2 * stage

    row_units = [slice(lo, lo + UNIT) for lo in range(0, width, UNIT)]

    def to_tile(rows):
        while rows.shape[0] > 8:
            mid = rows.shape[0] // 2
            rows = rows[:mid] + rows[mid:]
        return rows

    def mean_of(tiles_of_half):
        total = tiles_of_half[0::2]
        total = [a + b for a, b in zip(total, tiles_of_half[1::2])]
        while len(total) > 1:
            total = [a + b for a, b in zip(total[::2], total[1::2])] + total[len(total) - len(total) % 2:]
        return jnp.sum(total[0], axis=0, keepdims=True) * (1.0 / width)

    def norm_store(sums, scale_row, shift_row):
        stats = []
        for half, tiles_of_half in zip(halves, sums):
            mean = mean_of(tiles_of_half)
            squares = []
            for rows in row_units:
                centered = h_scr[rows, half] - mean
                squares.append(to_tile(centered * centered))
            stats.append((mean, lax.rsqrt(mean_of(squares) + LN_EPS)))
        for rows in row_units:
            for half, (mean, rstd) in zip(halves, stats):
                u_scr[rows, half] = ((h_scr[rows, half] - mean) * rstd * lanes[scale_row, rows] + lanes[shift_row, rows]).astype(bf16)

    quarter = width // 2
    each = quarter // UNIT

    row_units = [slice(lo, lo + UNIT) for lo in range(0, width, UNIT)]

    def to_tile(rows):
        while rows.shape[0] > 8:
            mid = rows.shape[0] // 2
            rows = rows[:mid] + rows[mid:]
        return rows

    def mean_of(tiles_of_half):
        total = tiles_of_half[0::2]
        total = [a + b for a, b in zip(total, tiles_of_half[1::2])]
        while len(total) > 1:
            total = [a + b for a, b in zip(total[::2], total[1::2])] + total[len(total) - len(total) % 2:]
        return jnp.sum(total[0], axis=0, keepdims=True) * (1.0 / width)

    def norm_store(sums, scale_row, shift_row):
        stats = []
        for half, tiles_of_half in zip(halves, sums):
            mean = mean_of(tiles_of_half)
            squares = []
            for rows in row_units:
                centered = h_scr[rows, half] - mean
                squares.append(to_tile(centered * centered))
            stats.append((mean, lax.rsqrt(mean_of(squares) + LN_EPS)))
        for rows in row_units:
            for half, (mean, rstd) in zip(halves, stats):
                u_scr[rows, half] = ((h_scr[rows, half] - mean) * rstd * lanes[scale_row, rows] + lanes[shift_row, rows]).astype(bf16)

    quarter = width // 2
    each = quarter // UNIT

    def tiles(rows):
        return rows[:256], jnp.concatenate([zeros_half, rows[256:]], axis=0)

    def weight(ref, row, register):
        lo = 0 if register == 0 else width - 256
        return ref[row:row + UNIT, lo:lo + 256]

    def block(step, hidden_in, beside=lambda: None, post=lambda: None):
        fills = {(pair, part): fill(step, pair, part) for pair in (1, 2) for part in range(parts)}
        sums = [[], []]
        for rows in row_units:
            for side, half in enumerate(halves):
                hidden = hidden_in(half, rows)
                h_scr[rows, half] = hidden
                sums[side].append(to_tile(hidden))
        norm_store(sums, 1, 0)
        normed = u_scr[...]
        pairs = heads // 2

        def project_in(kind, lo, hi):
            start = kind * width
            return dot(qkv_w[start + lo * head_dim:start + hi * head_dim], normed).astype(bf16)

        def per_head(rows):
            return [rows[lo:lo + head_dim] for lo in range(0, rows.shape[0], head_dim)]

        groups = ((0, 2), (2, heads))
        keys, queries = [], []
        for lo, hi in groups:
            keys += per_head(project_in(1, lo, hi))
            queries += per_head(project_in(0, lo, hi))
        for (pair, part), both in fills.items():
            store_fill(pair, part, both)
        factor = LOG2E * head_dim ** -0.5

        def score(index):
            return [dot(keys[head].T, queries[head]) for head in (2 * index, 2 * index + 1)]

        def softmax(scores):
            top = jnp.max(scores, axis=0, keepdims=True)
            expo = jnp.exp2((scores - top) * factor)
            return expo.astype(bf16), float(tokens) / fold(expo)

        beside()
        scores = [score(0)]
        values = per_head(project_in(2, 0, 2))
        scores.append(score(1))
        values += per_head(project_in(2, 2, heads))
        proj = [None, None]

        def project_out(lo, hi):
            for side in range(2):
                piece = dot(proj_w[side * quarter:side * quarter + quarter, lo:hi], o_scr[lo:hi])
                if lo == 0:
                    p_scr[side * quarter:side * quarter + quarter] = piece
                else:
                    proj[side] = piece

        for index in range(pairs):
            if index + 2 < pairs:
                scores.append(score(index + 2))
            outs = []
            for unit in range(2):
                head = 2 * index + unit
                done = [softmax(scores[index][unit][:, half]) for half in halves]
                inverse = jnp.concatenate([pair[1] for pair in done], axis=1)
                expo = jnp.concatenate([pair[0] for pair in done], axis=1)
                outs.append((dot(values[head], expo), inverse))
            if index == pairs - 1:
                project_out(0, 256)
                after = jnp.minimum(step + 1, steps - 1)
                for part in range(parts):
                    store_fill(0, part, fill(after, 0, part))
            for unit, (out, inverse) in enumerate(outs):
                head = 2 * index + unit
                o_scr[head * head_dim:(head + 1) * head_dim] = (out * inverse).astype(bf16)
        project_out(256, width)
        post()
        sums = [[], []]
        for unit in range(2):
            for part in range(each):
                lo = unit * quarter + part * UNIT
                rows = slice(lo, lo + UNIT)
                piece = proj[unit][part * UNIT:part * UNIT + UNIT] + p_scr[rows]
                for side, half in enumerate(halves):
                    hidden = h_scr[rows, half] + lanes[2, rows] * piece[:, half]
                    h_scr[rows, half] = hidden
                    sums[side].append(to_tile(hidden))
        norm_store(sums, 4, 3)
        normed = u_scr[...]
        tile_count = mlp // 256
        ups = [dot(up_w[tile * 256:tile * 256 + 256], normed) for tile in range(tile_count)]

        def gelu(pre):
            return (pre * jnp.tanh(pre * (2.0 * GELU_A + 8.0 * GELU_B * (pre * pre))) + pre).astype(bf16)

        down = [None, None]
        for tile in range(tile_count):
            act = jnp.concatenate([gelu(ups[tile][lo:lo + UNIT]) for lo in range(0, 256, UNIT)], axis=0)
            for side in range(2):
                piece = dot(down_w[side * quarter:side * quarter + quarter, tile * 256:tile * 256 + 256], act)
                down[side] = piece if down[side] is None else down[side] + piece
        for unit in range(2):
            for part in range(each):
                lo = unit * quarter + part * UNIT
                rows = slice(lo, lo + UNIT)
                for half in halves:
                    yield rows, half, h_scr[rows, half] + lanes[5, rows] * down[unit][part * UNIT:part * UNIT + UNIT, half]

    def send(step, columns):
        for rows, half, hidden in columns:
            sent[step, rows, half] = hidden.astype(bf16)
        hidden_copy(step).start()

    def received(step):
        return lambda half, rows=slice(None): recv[step, rows, half].astype(f32)

    def wait_hidden(step):
        @pl.when(step >= 2)
        def _():
            hidden_copy(step - 2).wait_recv()

    def first_step(step, carry):
        @pl.when(step >= 1)
        def _():
            latent_copy(step - 1).wait_recv()
        h_last[...] = dot(w_in_t[...], x_recv[step].astype(bf16))
        send(step, block(step, lambda half, rows=slice(None): h_last[rows, half]))
        return carry

    def middle_step(step, carry):
        wait_hidden(step)
        send(step, block(step, received(step)))
        return carry

    def advance(step):
        normed = jnp.concatenate([normalize(h_last[:, half]).astype(bf16) for half in halves], axis=1)
        noise = dot(w_out_ref[...], normed)
        x_next = keep_ref[step] * x_cur[...] + noise_ref[step] * noise
        x_cur[...] = x_next
        return x_next

    def last_step(sends, step, carry):
        wait_hidden(step)
        before = jnp.maximum(step - 1, 0)

        def beside():
            x_next = jnp.where(step > 0, advance(before), x_ref[...])
            x_cur[...] = x_next
            if sends:
                x_recv[step + 1] = x_next

        def post():
            if sends:
                latent_copy(step).start()

        for rows, half, hidden in block(step, received(step), beside, post):
            h_last[rows, half] = hidden
        return carry

    def final_copy(ahead):
        return pltpu.make_async_remote_copy(
            src_ref=x_cur, dst_ref=out_ref, send_sem=last_send_sem.at[ahead], recv_sem=last_recv_sem,
            device_id={'stage': lax.rem(stage + ahead, stages)}, device_id_type=MESH)

    @pl.when(is_first)
    def _():
        lax.fori_loop(0, first_trips, first_step, 0)

    @pl.when(jnp.logical_not(is_first | is_last))
    def _():
        lax.fori_loop(0, trips, middle_step, 0)

    @pl.when(is_last)
    def _():
        h_last[...] = jnp.zeros_like(h_last)
        lax.fori_loop(0, first_trips - 1, functools.partial(last_step, True), 0)
        lax.fori_loop(first_trips - 1, steps, functools.partial(last_step, False), 0)
        out_ref[...] = advance(steps - 1)
        for ahead in sorted(range(1, stages), key=lambda ahead: -min(ahead, stages - ahead)):
            final_copy(ahead).start()
        for ahead in range(1, stages):
            final_copy(ahead).wait_send()

        def drain(step, carry):
            latent_copy(step).wait_send()
            return carry
        lax.fori_loop(0, first_trips - 1, drain, 0)

    @pl.when(jnp.logical_not(is_last))
    def _():
        def drain(step, carry):
            hidden_copy(step).wait_send()
            return carry
        lax.fori_loop(0, trips, drain, 0)
        final_copy(1).wait_recv()


def solution(mesh):
    stages = mesh.shape['stage']

    def shard_body(x_init, w_in, w_out, w_qkv, w_proj, w_up, w_down, mod_table, coef_keep, coef_noise, h_warm):
        steps = coef_keep.shape[0]
        tokens, chan = x_init.shape[1], x_init.shape[2]
        width, mlp = w_up.shape[1], w_up.shape[2]
        heads, head_dim = w_proj.shape[1], w_proj.shape[2]
        mod_rows = mod_table.shape[2] * width // 128
        bf16, f32 = jnp.bfloat16, jnp.float32
        vmem = pl.BlockSpec(memory_space=pltpu.VMEM)
        smem = pl.BlockSpec(memory_space=pltpu.SMEM)
        hbm = pl.BlockSpec(memory_space=pl.ANY)
        out = pl.pallas_call(
            functools.partial(kernel, stages),
            out_shape=jax.ShapeDtypeStruct((chan, tokens), f32),
            in_specs=[hbm] * 8 + [smem, smem, hbm],
            out_specs=vmem,
            scratch_shapes=[
                pltpu.VMEM((chan, tokens), f32),
                pltpu.VMEM((chan, width), bf16),
                pltpu.VMEM((chan, width), bf16),
                pltpu.VMEM((steps * mod_rows, 128), f32),
                pltpu.VMEM((width, 3 * width), bf16),
                pltpu.VMEM((heads, head_dim, width), bf16),
                pltpu.VMEM((width, mlp), bf16),
                pltpu.VMEM((mlp, width), bf16),
                pltpu.VMEM((2, tokens, width), bf16),
                pltpu.VMEM((width, chan), bf16),
                pltpu.VMEM((3 * width, width), bf16),
                pltpu.VMEM((width, width), bf16),
                pltpu.VMEM((mlp, width), bf16),
                pltpu.VMEM((width, mlp), bf16),
                pltpu.VMEM((steps, 128, 128), bf16),
                pltpu.VMEM((3 * width // 128, 128, 256), bf16),
                pltpu.VMEM((6, width, 128), f32),
                pltpu.VMEM((steps, width, tokens), bf16),
                pltpu.VMEM((steps, width, tokens), bf16),
                pltpu.VMEM((steps, chan, tokens), f32),
                pltpu.VMEM((chan, tokens), f32),
                pltpu.VMEM((width, tokens), f32),
                pltpu.VMEM((width, tokens), f32),
                pltpu.VMEM((width, tokens), bf16),
                pltpu.VMEM((width, tokens), bf16),
                pltpu.VMEM((width, tokens), f32),
                pltpu.SemaphoreType.DMA((9,)),
                pltpu.SemaphoreType.DMA((steps,)),
                pltpu.SemaphoreType.DMA((steps,)),
                pltpu.SemaphoreType.DMA((steps,)),
                pltpu.SemaphoreType.DMA((steps,)),
                pltpu.SemaphoreType.DMA((stages,)),
                pltpu.SemaphoreType.DMA,
            ],
            compiler_params=pltpu.CompilerParams(collective_id=0, has_side_effects=True, vmem_limit_bytes=56 * 1024 * 1024),
            name='stage_loop',
        )(jnp.swapaxes(x_init, 1, 2)[0], w_in, jnp.swapaxes(w_out, 0, 1), w_qkv[0], w_proj[0], w_up[0], w_down[0],
          mod_table.reshape(steps * mod_rows, 128), coef_keep, coef_noise, h_warm)
        return jnp.swapaxes(out, 0, 1)[None]

    return jax.shard_map(
        shard_body,
        mesh=mesh,
        in_specs=(P('data'), P(), P(), P('stage'), P('stage'), P('stage'), P('stage'), P(None, 'stage'), P(), P(), P(None, None, 'data')),
        out_specs=P('data'),
        check_vma=False,
    )
```

```python
import functools
import math

import jax
import jax.numpy as jnp
from jax import lax
from jax.experimental import pallas as pl
from jax.experimental.pallas import tpu as pltpu
from jax.sharding import PartitionSpec as P

LN_EPS = 1e-6
LOG2E = math.log2(math.e)
GELU_A = math.sqrt(2.0 / math.pi)
GELU_B = GELU_A * 0.044715
UNIT = 32
MESH = pl.DeviceIdType.MESH


def fold(rows):
    while rows.shape[0] % 16 == 0:
        half = rows.shape[0] // 2
        rows = rows[:half] + rows[half:]
    parts = [rows[lo:lo + 8] for lo in range(0, rows.shape[0], 8)]
    while len(parts) > 1:
        parts = [a + b for a, b in zip(parts[::2], parts[1::2])] + parts[len(parts) - len(parts) % 2:]
    return jnp.sum(parts[0], axis=0, keepdims=True)


def normalize(hidden):
    scale = 1.0 / hidden.shape[0]
    centered = hidden - fold(hidden) * scale
    var = fold(centered * centered) * scale
    return centered * lax.rsqrt(var + LN_EPS)


def dot(lhs, rhs):
    return jnp.dot(lhs, rhs, preferred_element_type=jnp.float32)


def kernel(stages, x_hbm, w_in_hbm, w_out_hbm, qkv_hbm, proj_hbm, up_hbm, down_hbm, mod_hbm, keep_ref, noise_ref, warm_hbm,
           out_ref, x_ref, w_in_ref, w_out_ref, mod_ref, qkv_n, proj_n, up_n, down_n, warm_n, w_in_t, qkv_w, proj_w, up_w, down_w, mod_s, select, lanes,
           recv, sent, x_recv, x_cur, h_last, h_scr, u_scr, o_scr, p_scr, load_sem, recv_sem, send_sem, x_recv_sem, x_send_sem, last_send_sem, last_recv_sem):
    stage = lax.axis_index('stage')
    is_first = stage == 0
    is_last = stage == stages - 1
    steps = keep_ref.shape[0]
    width, tokens = h_last.shape
    heads, head_dim = proj_hbm.shape[0], proj_hbm.shape[1]
    mlp = up_w.shape[0]
    bf16, f32 = jnp.bfloat16, jnp.float32

    loads = [
        pltpu.make_async_copy(warm_hbm.at[:, jnp.maximum(stage - 1, 0), 0], warm_n, load_sem.at[0]),
        pltpu.make_async_copy(qkv_hbm, qkv_n, load_sem.at[1]),
        pltpu.make_async_copy(proj_hbm, proj_n, load_sem.at[2]),
        pltpu.make_async_copy(up_hbm, up_n, load_sem.at[3]),
        pltpu.make_async_copy(down_hbm, down_n, load_sem.at[4]),
        pltpu.make_async_copy(x_hbm, x_ref, load_sem.at[5]),
        pltpu.make_async_copy(w_in_hbm, w_in_ref, load_sem.at[6]),
        pltpu.make_async_copy(w_out_hbm, w_out_ref, load_sem.at[7]),
        pltpu.make_async_copy(mod_hbm, mod_ref, load_sem.at[8]),
    ]
    for index in (8, 5, 6, 7, 0, 1, 2, 3, 4):
        loads[index].start()
    barrier = pltpu.get_barrier_semaphore()
    for ahead in range(1, stages):
        pl.semaphore_signal(barrier, inc=1, device_id={'stage': lax.rem(stage + ahead, stages)}, device_id_type=MESH)

    loads[8].wait()
    mod_rows = mod_ref.shape[0] // steps
    parts = width // 128
    pad = mod_rows + -mod_rows % 8
    row_id = lax.broadcasted_iota(jnp.int32, (mod_rows, 128), 0) // parts
    plus = jnp.where((row_id == 1) | (row_id == 4), 1.0, 0.0)
    limit = float(jnp.finfo(bf16).max)
    gap = jnp.zeros((pad - mod_rows, 128), f32)
    rest_rows = jnp.zeros((128 - 3 * pad, 128), f32)

    for step in range(steps):
        rows = mod_ref[step * mod_rows:(step + 1) * mod_rows] + plus
        high = jnp.clip(rows, -limit, limit).astype(bf16).astype(f32)
        rest = rows - high
        mid = rest.astype(bf16).astype(f32)
        terms = jnp.concatenate([high, gap, mid, gap, rest - mid, gap, rest_rows], axis=0)
        mod_s[step] = terms.T.astype(bf16)

    term = lax.broadcasted_iota(jnp.int32, (128, 256), 0)
    term = jnp.where(term < 3 * pad, term % pad, -1)
    column = lax.broadcasted_iota(jnp.int32, (128, 256), 1) // 128
    for pair in range(3):
        for part in range(parts):
            pick = term == (2 * pair + column) * parts + part
            select[pair * parts + part] = jnp.where(pick, 1.0, 0.0).astype(bf16)

    def fill(step, pair, part):
        return dot(mod_s[step], select[pair * parts + part])

    def store_fill(pair, part, both):
        for side in range(2):
            lanes[2 * pair + side, part * 128:part * 128 + 128] = both[:, side * 128:side * 128 + 128]

    halves = [slice(lo, lo + 128) for lo in range(0, tokens, 128)]

    for index in (5, 6, 7):
        loads[index].wait()
    w_in_t[...] = w_in_ref[...].T
    x_cur[...] = x_ref[...]
    x_recv[0] = x_ref[...]
    for index in range(5):
        loads[index].wait()
    for slot in range(2):
        recv[slot] = warm_n[slot].T
    qkv_w[:2 * width] = qkv_n[:, :2 * width].T
    qkv_w[2 * width:] = qkv_n[:, 2 * width:].T * jnp.asarray(1.0 / tokens, bf16)
    proj_w[...] = proj_n[...].reshape(width, width).T
    up_w[...] = up_n[...].T * jnp.asarray(0.5, bf16)
    down_w[...] = down_n[...].T
    for part in range(parts):
        store_fill(0, part, fill(0, 0, part))
    pl.semaphore_wait(barrier, stages - 1)

    next_id = {'stage': lax.rem(stage + 1, stages)}

    def hidden_copy(step):
        return pltpu.make_async_remote_copy(
            src_ref=sent.at[step], dst_ref=recv.at[step + 2], send_sem=send_sem.at[step], recv_sem=recv_sem.at[step + 2],
            device_id=next_id, device_id_type=MESH)

    def latent_copy(step):
        return pltpu.make_async_remote_copy(
            src_ref=x_recv.at[step + 1], dst_ref=x_recv.at[step + 1], send_sem=x_send_sem.at[step], recv_sem=x_recv_sem.at[step],
            device_id=next_id, device_id_type=MESH)

    first_trips = steps - 2 * (stages - 1)
    trips = first_trips + 2 * stage

    row_units = [slice(lo, lo + UNIT) for lo in range(0, width, UNIT)]

    def to_tile(rows):
        while rows.shape[0] > 8:
            mid = rows.shape[0] // 2
            rows = rows[:mid] + rows[mid:]
        return rows

    def mean_of(tiles_of_half):
        total = tiles_of_half[0::2]
        total = [a + b for a, b in zip(total, tiles_of_half[1::2])]
        while len(total) > 1:
            total = [a + b for a, b in zip(total[::2], total[1::2])] + total[len(total) - len(total) % 2:]
        return jnp.sum(total[0], axis=0, keepdims=True) * (1.0 / width)

    def norm_store(sums, scale_row, shift_row):
        stats = []
        for half, tiles_of_half in zip(halves, sums):
            mean = mean_of(tiles_of_half)
            squares = []
            for rows in row_units:
                centered = h_scr[rows, half] - mean
                squares.append(to_tile(centered * centered))
            stats.append((mean, lax.rsqrt(mean_of(squares) + LN_EPS)))
        for rows in row_units:
            for half, (mean, rstd) in zip(halves, stats):
                u_scr[rows, half] = ((h_scr[rows, half] - mean) * rstd * lanes[scale_row, rows] + lanes[shift_row, rows]).astype(bf16)

    quarter = width // 2
    each = quarter // UNIT

    row_units = [slice(lo, lo + UNIT) for lo in range(0, width, UNIT)]

    def to_tile(rows):
        while rows.shape[0] > 8:
            mid = rows.shape[0] // 2
            rows = rows[:mid] + rows[mid:]
        return rows

    def mean_of(tiles_of_half):
        total = tiles_of_half[0::2]
        total = [a + b for a, b in zip(total, tiles_of_half[1::2])]
        while len(total) > 1:
            total = [a + b for a, b in zip(total[::2], total[1::2])] + total[len(total) - len(total) % 2:]
        return jnp.sum(total[0], axis=0, keepdims=True) * (1.0 / width)

    def norm_store(sums, scale_row, shift_row):
        stats = []
        for half, tiles_of_half in zip(halves, sums):
            mean = mean_of(tiles_of_half)
            squares = []
            for rows in row_units:
                centered = h_scr[rows, half] - mean
                squares.append(to_tile(centered * centered))
            stats.append((mean, lax.rsqrt(mean_of(squares) + LN_EPS)))
        for rows in row_units:
            for half, (mean, rstd) in zip(halves, stats):
                u_scr[rows, half] = ((h_scr[rows, half] - mean) * rstd * lanes[scale_row, rows] + lanes[shift_row, rows]).astype(bf16)

    quarter = width // 2
    each = quarter // UNIT

    def tiles(rows):
        return rows[:256], jnp.concatenate([zeros_half, rows[256:]], axis=0)

    def weight(ref, row, register):
        lo = 0 if register == 0 else width - 256
        return ref[row:row + UNIT, lo:lo + 256]

    def block(step, hidden_in, beside=lambda: None, post=lambda: None):
        fills = {(pair, part): fill(step, pair, part) for pair in (1, 2) for part in range(parts)}
        sums = [[], []]
        for rows in row_units:
            for side, half in enumerate(halves):
                hidden = hidden_in(half, rows)
                h_scr[rows, half] = hidden
                sums[side].append(to_tile(hidden))
        norm_store(sums, 1, 0)
        normed = u_scr[...]
        pairs = heads // 2

        def project_in(kind, lo, hi):
            start = kind * width
            return dot(qkv_w[start + lo * head_dim:start + hi * head_dim], normed).astype(bf16)

        def per_head(rows):
            return [rows[lo:lo + head_dim] for lo in range(0, rows.shape[0], head_dim)]

        groups = ((0, 2), (2, heads))
        keys, queries = [], []
        for lo, hi in groups:
            keys += per_head(project_in(1, lo, hi))
            queries += per_head(project_in(0, lo, hi))
        for (pair, part), both in fills.items():
            store_fill(pair, part, both)
        factor = LOG2E * head_dim ** -0.5

        def score(index):
            return [dot(keys[head].T, queries[head]) for head in (2 * index, 2 * index + 1)]

        def softmax(scores):
            best = scores
            while best.shape[0] > 8:
                best = jnp.maximum(best[:best.shape[0] // 2], best[best.shape[0] // 2:])
            top = jnp.max(best, axis=0, keepdims=True)
            expo = jnp.exp2((scores - top) * factor)
            return expo.astype(bf16), float(tokens) / jnp.sum(expo, axis=0, keepdims=True)

        beside()
        scores = [score(0)]
        values = per_head(project_in(2, 0, 2))
        scores.append(score(1))
        values += per_head(project_in(2, 2, heads))
        proj = [None, None]

        def project_out(lo, hi):
            for side in range(2):
                piece = dot(proj_w[side * quarter:side * quarter + quarter, lo:hi], o_scr[lo:hi])
                if lo == 0:
                    p_scr[side * quarter:side * quarter + quarter] = piece
                else:
                    proj[side] = piece

        for index in range(pairs):
            if index + 2 < pairs:
                scores.append(score(index + 2))
            outs = []
            for unit in range(2):
                head = 2 * index + unit
                done = [softmax(scores[index][unit][:, half]) for half in halves]
                inverse = jnp.concatenate([pair[1] for pair in done], axis=1)
                expo = jnp.concatenate([pair[0] for pair in done], axis=1)
                outs.append((dot(values[head], expo), inverse))
            if index == pairs - 1:
                project_out(0, 256)
                after = jnp.minimum(step + 1, steps - 1)
                for part in range(parts):
                    store_fill(0, part, fill(after, 0, part))
            for unit, (out, inverse) in enumerate(outs):
                head = 2 * index + unit
                o_scr[head * head_dim:(head + 1) * head_dim] = (out * inverse).astype(bf16)
        project_out(256, width)
        post()
        sums = [[], []]
        for part in range(each):
            for unit in range(2):
                lo = unit * quarter + part * UNIT
                rows = slice(lo, lo + UNIT)
                piece = proj[unit][part * UNIT:part * UNIT + UNIT] + p_scr[rows]
                for side, half in enumerate(halves):
                    hidden = h_scr[rows, half] + lanes[2, rows] * piece[:, half]
                    h_scr[rows, half] = hidden
                    sums[side].append(to_tile(hidden))
        norm_store(sums, 4, 3)
        normed = u_scr[...]
        tile_count = mlp // 256
        ups = [dot(up_w[tile * 256:tile * 256 + 256], normed) for tile in range(tile_count)]

        def gelu(pre):
            return (pre * jnp.tanh(pre * (2.0 * GELU_A + 8.0 * GELU_B * (pre * pre))) + pre).astype(bf16)

        down = [None, None]
        for tile in range(tile_count):
            act = jnp.concatenate([gelu(ups[tile][lo:lo + UNIT]) for lo in range(0, 256, UNIT)], axis=0)
            for side in range(2):
                piece = dot(down_w[side * quarter:side * quarter + quarter, tile * 256:tile * 256 + 256], act)
                down[side] = piece if down[side] is None else down[side] + piece
        for unit in range(2):
            for part in range(each):
                lo = unit * quarter + part * UNIT
                rows = slice(lo, lo + UNIT)
                for half in halves:
                    yield rows, half, h_scr[rows, half] + lanes[5, rows] * down[unit][part * UNIT:part * UNIT + UNIT, half]

    def send(step, columns):
        for rows, half, hidden in columns:
            sent[step, rows, half] = hidden.astype(bf16)
        hidden_copy(step).start()

    def received(step):
        return lambda half, rows=slice(None): recv[step, rows, half].astype(f32)

    def wait_hidden(step):
        @pl.when(step >= 2)
        def _():
            hidden_copy(step - 2).wait_recv()

    def first_step(step, carry):
        @pl.when(step >= 1)
        def _():
            latent_copy(step - 1).wait_recv()
        h_last[...] = dot(w_in_t[...], x_recv[step].astype(bf16))
        send(step, block(step, lambda half, rows=slice(None): h_last[rows, half]))
        return carry

    def middle_step(step, carry):
        wait_hidden(step)
        send(step, block(step, received(step)))
        return carry

    def advance(step):
        normed = jnp.concatenate([normalize(h_last[:, half]).astype(bf16) for half in halves], axis=1)
        noise = dot(w_out_ref[...], normed)
        x_next = keep_ref[step] * x_cur[...] + noise_ref[step] * noise
        x_cur[...] = x_next
        return x_next

    def last_step(sends, step, carry):
        wait_hidden(step)
        before = jnp.maximum(step - 1, 0)

        def beside():
            x_next = jnp.where(step > 0, advance(before), x_ref[...])
            x_cur[...] = x_next
            if sends:
                x_recv[step + 1] = x_next

        def post():
            if sends:
                latent_copy(step).start()

        for rows, half, hidden in block(step, received(step), beside, post):
            h_last[rows, half] = hidden
        return carry

    def final_copy(ahead):
        return pltpu.make_async_remote_copy(
            src_ref=x_cur, dst_ref=out_ref, send_sem=last_send_sem.at[ahead], recv_sem=last_recv_sem,
            device_id={'stage': lax.rem(stage + ahead, stages)}, device_id_type=MESH)

    @pl.when(is_first)
    def _():
        lax.fori_loop(0, first_trips, first_step, 0)

    @pl.when(jnp.logical_not(is_first | is_last))
    def _():
        lax.fori_loop(0, trips, middle_step, 0)

    @pl.when(is_last)
    def _():
        h_last[...] = jnp.zeros_like(h_last)
        lax.fori_loop(0, first_trips - 1, functools.partial(last_step, True), 0)
        lax.fori_loop(first_trips - 1, steps, functools.partial(last_step, False), 0)
        out_ref[...] = advance(steps - 1)
        for ahead in sorted(range(1, stages), key=lambda ahead: -min(ahead, stages - ahead)):
            final_copy(ahead).start()
        for ahead in range(1, stages):
            final_copy(ahead).wait_send()

        def drain(step, carry):
            latent_copy(step).wait_send()
            return carry
        lax.fori_loop(0, first_trips - 1, drain, 0)

    @pl.when(jnp.logical_not(is_last))
    def _():
        def drain(step, carry):
            hidden_copy(step).wait_send()
            return carry
        lax.fori_loop(0, trips, drain, 0)
        final_copy(1).wait_recv()


def solution(mesh):
    stages = mesh.shape['stage']

    def shard_body(x_init, w_in, w_out, w_qkv, w_proj, w_up, w_down, mod_table, coef_keep, coef_noise, h_warm):
        steps = coef_keep.shape[0]
        tokens, chan = x_init.shape[1], x_init.shape[2]
        width, mlp = w_up.shape[1], w_up.shape[2]
        heads, head_dim = w_proj.shape[1], w_proj.shape[2]
        mod_rows = mod_table.shape[2] * width // 128
        bf16, f32 = jnp.bfloat16, jnp.float32
        vmem = pl.BlockSpec(memory_space=pltpu.VMEM)
        smem = pl.BlockSpec(memory_space=pltpu.SMEM)
        hbm = pl.BlockSpec(memory_space=pl.ANY)
        out = pl.pallas_call(
            functools.partial(kernel, stages),
            out_shape=jax.ShapeDtypeStruct((chan, tokens), f32),
            in_specs=[hbm] * 8 + [smem, smem, hbm],
            out_specs=vmem,
            scratch_shapes=[
                pltpu.VMEM((chan, tokens), f32),
                pltpu.VMEM((chan, width), bf16),
                pltpu.VMEM((chan, width), bf16),
                pltpu.VMEM((steps * mod_rows, 128), f32),
                pltpu.VMEM((width, 3 * width), bf16),
                pltpu.VMEM((heads, head_dim, width), bf16),
                pltpu.VMEM((width, mlp), bf16),
                pltpu.VMEM((mlp, width), bf16),
                pltpu.VMEM((2, tokens, width), bf16),
                pltpu.VMEM((width, chan), bf16),
                pltpu.VMEM((3 * width, width), bf16),
                pltpu.VMEM((width, width), bf16),
                pltpu.VMEM((mlp, width), bf16),
                pltpu.VMEM((width, mlp), bf16),
                pltpu.VMEM((steps, 128, 128), bf16),
                pltpu.VMEM((3 * width // 128, 128, 256), bf16),
                pltpu.VMEM((6, width, 128), f32),
                pltpu.VMEM((steps, width, tokens), bf16),
                pltpu.VMEM((steps, width, tokens), bf16),
                pltpu.VMEM((steps, chan, tokens), f32),
                pltpu.VMEM((chan, tokens), f32),
                pltpu.VMEM((width, tokens), f32),
                pltpu.VMEM((width, tokens), f32),
                pltpu.VMEM((width, tokens), bf16),
                pltpu.VMEM((width, tokens), bf16),
                pltpu.VMEM((width, tokens), f32),
                pltpu.SemaphoreType.DMA((9,)),
                pltpu.SemaphoreType.DMA((steps,)),
                pltpu.SemaphoreType.DMA((steps,)),
                pltpu.SemaphoreType.DMA((steps,)),
                pltpu.SemaphoreType.DMA((steps,)),
                pltpu.SemaphoreType.DMA((stages,)),
                pltpu.SemaphoreType.DMA,
            ],
            compiler_params=pltpu.CompilerParams(collective_id=0, has_side_effects=True, vmem_limit_bytes=56 * 1024 * 1024),
            name='stage_loop',
        )(jnp.swapaxes(x_init, 1, 2)[0], w_in, jnp.swapaxes(w_out, 0, 1), w_qkv[0], w_proj[0], w_up[0], w_down[0],
          mod_table.reshape(steps * mod_rows, 128), coef_keep, coef_noise, h_warm)
        return jnp.swapaxes(out, 0, 1)[None]

    return jax.shard_map(
        shard_body,
        mesh=mesh,
        in_specs=(P('data'), P(), P(), P('stage'), P('stage'), P('stage'), P('stage'), P(None, 'stage'), P(), P(), P(None, None, 'data')),
        out_specs=P('data'),
        check_vma=False,
    )
```

```python
import functools
import math

import jax
import jax.numpy as jnp
from jax import lax
from jax.experimental import pallas as pl
from jax.experimental.pallas import tpu as pltpu
from jax.sharding import PartitionSpec as P

LN_EPS = 1e-6
LOG2E = math.log2(math.e)
GELU_A = math.sqrt(2.0 / math.pi)
GELU_B = GELU_A * 0.044715
UNIT = 32
MESH = pl.DeviceIdType.MESH


def fold(rows):
    while rows.shape[0] % 16 == 0:
        half = rows.shape[0] // 2
        rows = rows[:half] + rows[half:]
    parts = [rows[lo:lo + 8] for lo in range(0, rows.shape[0], 8)]
    while len(parts) > 1:
        parts = [a + b for a, b in zip(parts[::2], parts[1::2])] + parts[len(parts) - len(parts) % 2:]
    return jnp.sum(parts[0], axis=0, keepdims=True)


def normalize(hidden):
    scale = 1.0 / hidden.shape[0]
    centered = hidden - fold(hidden) * scale
    var = fold(centered * centered) * scale
    return centered * lax.rsqrt(var + LN_EPS)


def dot(lhs, rhs):
    return jnp.dot(lhs, rhs, preferred_element_type=jnp.float32)


def kernel(stages, x_hbm, w_in_hbm, w_out_hbm, qkv_hbm, proj_hbm, up_hbm, down_hbm, mod_hbm, keep_ref, noise_ref, warm_hbm,
           out_ref, x_ref, w_in_ref, w_out_ref, mod_ref, qkv_n, proj_n, up_n, down_n, warm_n, w_in_t, qkv_w, proj_w, up_w, down_w, mod_s, select, lanes,
           recv, sent, x_recv, x_cur, h_last, h_scr, u_scr, o_scr, p_scr, load_sem, recv_sem, send_sem, x_recv_sem, x_send_sem, last_send_sem, last_recv_sem):
    stage = lax.axis_index('stage')
    is_first = stage == 0
    is_last = stage == stages - 1
    steps = keep_ref.shape[0]
    width, tokens = h_last.shape
    heads, head_dim = proj_hbm.shape[0], proj_hbm.shape[1]
    mlp = up_w.shape[0]
    bf16, f32 = jnp.bfloat16, jnp.float32

    loads = [
        pltpu.make_async_copy(warm_hbm.at[:, jnp.maximum(stage - 1, 0), 0], warm_n, load_sem.at[0]),
        pltpu.make_async_copy(qkv_hbm, qkv_n, load_sem.at[1]),
        pltpu.make_async_copy(proj_hbm, proj_n, load_sem.at[2]),
        pltpu.make_async_copy(up_hbm, up_n, load_sem.at[3]),
        pltpu.make_async_copy(down_hbm, down_n, load_sem.at[4]),
        pltpu.make_async_copy(x_hbm, x_ref, load_sem.at[5]),
        pltpu.make_async_copy(w_in_hbm, w_in_ref, load_sem.at[6]),
        pltpu.make_async_copy(w_out_hbm, w_out_ref, load_sem.at[7]),
        pltpu.make_async_copy(mod_hbm, mod_ref, load_sem.at[8]),
    ]
    for index in (8, 5, 6, 7, 0, 1, 2, 3, 4):
        loads[index].start()
    barrier = pltpu.get_barrier_semaphore()
    for ahead in range(1, stages):
        pl.semaphore_signal(barrier, inc=1, device_id={'stage': lax.rem(stage + ahead, stages)}, device_id_type=MESH)

    loads[8].wait()
    mod_rows = mod_ref.shape[0] // steps
    parts = width // 128
    pad = mod_rows + -mod_rows % 8
    row_id = lax.broadcasted_iota(jnp.int32, (mod_rows, 128), 0) // parts
    plus = jnp.where((row_id == 1) | (row_id == 4), 1.0, 0.0)
    limit = float(jnp.finfo(bf16).max)
    gap = jnp.zeros((pad - mod_rows, 128), f32)
    rest_rows = jnp.zeros((128 - 3 * pad, 128), f32)

    for step in range(steps):
        rows = mod_ref[step * mod_rows:(step + 1) * mod_rows] + plus
        high = jnp.clip(rows, -limit, limit).astype(bf16).astype(f32)
        rest = rows - high
        mid = rest.astype(bf16).astype(f32)
        terms = jnp.concatenate([high, gap, mid, gap, rest - mid, gap, rest_rows], axis=0)
        mod_s[step] = terms.T.astype(bf16)

    term = lax.broadcasted_iota(jnp.int32, (128, 256), 0)
    term = jnp.where(term < 3 * pad, term % pad, -1)
    column = lax.broadcasted_iota(jnp.int32, (128, 256), 1) // 128
    for pair in range(3):
        for part in range(parts):
            pick = term == (2 * pair + column) * parts + part
            select[pair * parts + part] = jnp.where(pick, 1.0, 0.0).astype(bf16)

    def fill(step, pair, part):
        return dot(mod_s[step], select[pair * parts + part])

    def store_fill(pair, part, both):
        for side in range(2):
            lanes[2 * pair + side, part * 128:part * 128 + 128] = both[:, side * 128:side * 128 + 128]

    halves = [slice(lo, lo + 128) for lo in range(0, tokens, 128)]

    for index in (5, 6, 7):
        loads[index].wait()
    w_in_t[...] = w_in_ref[...].T
    x_cur[...] = x_ref[...]
    x_recv[0] = x_ref[...]
    for index in range(5):
        loads[index].wait()
    for slot in range(2):
        recv[slot] = warm_n[slot].T
    qkv_w[:2 * width] = qkv_n[:, :2 * width].T
    qkv_w[2 * width:] = qkv_n[:, 2 * width:].T * jnp.asarray(1.0 / tokens, bf16)
    proj_w[...] = proj_n[...].reshape(width, width).T
    up_w[...] = up_n[...].T * jnp.asarray(0.5, bf16)
    down_w[...] = down_n[...].T
    for part in range(parts):
        store_fill(0, part, fill(0, 0, part))
    pl.semaphore_wait(barrier, stages - 1)

    next_id = {'stage': lax.rem(stage + 1, stages)}

    def hidden_copy(step):
        return pltpu.make_async_remote_copy(
            src_ref=sent.at[step], dst_ref=recv.at[step + 2], send_sem=send_sem.at[step], recv_sem=recv_sem.at[step + 2],
            device_id=next_id, device_id_type=MESH)

    def latent_copy(step):
        return pltpu.make_async_remote_copy(
            src_ref=x_recv.at[step + 1], dst_ref=x_recv.at[step + 1], send_sem=x_send_sem.at[step], recv_sem=x_recv_sem.at[step],
            device_id=next_id, device_id_type=MESH)

    first_trips = steps - 2 * (stages - 1)
    trips = first_trips + 2 * stage

    row_units = [slice(lo, lo + UNIT) for lo in range(0, width, UNIT)]

    def to_tile(rows):
        while rows.shape[0] > 8:
            mid = rows.shape[0] // 2
            rows = rows[:mid] + rows[mid:]
        return rows

    def mean_of(tiles_of_half):
        total = tiles_of_half[0::2]
        total = [a + b for a, b in zip(total, tiles_of_half[1::2])]
        while len(total) > 1:
            total = [a + b for a, b in zip(total[::2], total[1::2])] + total[len(total) - len(total) % 2:]
        return jnp.sum(total[0], axis=0, keepdims=True) * (1.0 / width)

    def norm_store(sums, scale_row, shift_row):
        stats = []
        for half, tiles_of_half in zip(halves, sums):
            mean = mean_of(tiles_of_half)
            squares = []
            for rows in row_units:
                centered = h_scr[rows, half] - mean
                squares.append(to_tile(centered * centered))
            stats.append((mean, lax.rsqrt(mean_of(squares) + LN_EPS)))
        for rows in row_units:
            for half, (mean, rstd) in zip(halves, stats):
                u_scr[rows, half] = ((h_scr[rows, half] - mean) * rstd * lanes[scale_row, rows] + lanes[shift_row, rows]).astype(bf16)

    quarter = width // 2
    each = quarter // UNIT

    row_units = [slice(lo, lo + UNIT) for lo in range(0, width, UNIT)]

    def to_tile(rows):
        while rows.shape[0] > 8:
            mid = rows.shape[0] // 2
            rows = rows[:mid] + rows[mid:]
        return rows

    def mean_of(tiles_of_half):
        total = tiles_of_half[0::2]
        total = [a + b for a, b in zip(total, tiles_of_half[1::2])]
        while len(total) > 1:
            total = [a + b for a, b in zip(total[::2], total[1::2])] + total[len(total) - len(total) % 2:]
        return jnp.sum(total[0], axis=0, keepdims=True) * (1.0 / width)

    def norm_store(sums, scale_row, shift_row):
        stats = []
        for half, tiles_of_half in zip(halves, sums):
            mean = mean_of(tiles_of_half)
            squares = []
            for rows in row_units:
                centered = h_scr[rows, half] - mean
                squares.append(to_tile(centered * centered))
            stats.append((mean, lax.rsqrt(mean_of(squares) + LN_EPS)))
        for rows in row_units:
            for half, (mean, rstd) in zip(halves, stats):
                u_scr[rows, half] = ((h_scr[rows, half] - mean) * rstd * lanes[scale_row, rows] + lanes[shift_row, rows]).astype(bf16)

    quarter = width // 2
    each = quarter // UNIT

    def tiles(rows):
        return rows[:256], jnp.concatenate([zeros_half, rows[256:]], axis=0)

    def weight(ref, row, register):
        lo = 0 if register == 0 else width - 256
        return ref[row:row + UNIT, lo:lo + 256]

    def block(step, hidden_in, beside=lambda: None, post=lambda: None):
        fills = {(pair, part): fill(step, pair, part) for pair in (1, 2) for part in range(parts)}
        sums = [[], []]
        for rows in row_units:
            for side, half in enumerate(halves):
                hidden = hidden_in(half, rows)
                h_scr[rows, half] = hidden
                sums[side].append(to_tile(hidden))
        norm_store(sums, 1, 0)
        normed = u_scr[...]
        pairs = heads // 2

        def project_in(kind, lo, hi):
            start = kind * width
            return dot(qkv_w[start + lo * head_dim:start + hi * head_dim], normed).astype(bf16)

        def per_head(rows):
            return [rows[lo:lo + head_dim] for lo in range(0, rows.shape[0], head_dim)]

        groups = ((0, 2), (2, heads))
        keys, queries = [], []
        for lo, hi in groups:
            keys += per_head(project_in(1, lo, hi))
            queries += per_head(project_in(0, lo, hi))
        for (pair, part), both in fills.items():
            store_fill(pair, part, both)
        factor = LOG2E * head_dim ** -0.5

        def score(index):
            return [dot(keys[head].T, queries[head]) for head in (2 * index, 2 * index + 1)]

        def softmax(scores):
            best = scores
            while best.shape[0] > 8:
                best = jnp.maximum(best[:best.shape[0] // 2], best[best.shape[0] // 2:])
            top = jnp.max(best, axis=0, keepdims=True)
            expo = jnp.exp2((scores - top) * factor)
            return expo.astype(bf16), float(tokens) / jnp.sum(expo, axis=0, keepdims=True)

        beside()
        scores = [score(0)]
        values = per_head(project_in(2, 0, 4))
        scores.append(score(1))
        values += per_head(project_in(2, 4, heads))
        proj = [None, None]

        def project_out(lo, hi):
            for side in range(2):
                piece = dot(proj_w[side * quarter:side * quarter + quarter, lo:hi], o_scr[lo:hi])
                if lo == 0:
                    p_scr[side * quarter:side * quarter + quarter] = piece
                else:
                    proj[side] = piece

        for index in range(pairs):
            if index + 2 < pairs:
                scores.append(score(index + 2))
            outs = []
            for unit in range(2):
                head = 2 * index + unit
                done = [softmax(scores[index][unit][:, half]) for half in halves]
                inverse = jnp.concatenate([pair[1] for pair in done], axis=1)
                expo = jnp.concatenate([pair[0] for pair in done], axis=1)
                outs.append((dot(values[head], expo), inverse))
            if index == pairs - 1:
                project_out(0, 256)
                after = jnp.minimum(step + 1, steps - 1)
                for part in range(parts):
                    store_fill(0, part, fill(after, 0, part))
            for unit, (out, inverse) in enumerate(outs):
                head = 2 * index + unit
                o_scr[head * head_dim:(head + 1) * head_dim] = (out * inverse).astype(bf16)
        project_out(256, width)
        post()
        sums = [[], []]
        for part in range(each):
            for unit in range(2):
                lo = unit * quarter + part * UNIT
                rows = slice(lo, lo + UNIT)
                piece = proj[unit][part * UNIT:part * UNIT + UNIT] + p_scr[rows]
                for side, half in enumerate(halves):
                    hidden = h_scr[rows, half] + lanes[2, rows] * piece[:, half]
                    h_scr[rows, half] = hidden
                    sums[side].append(to_tile(hidden))
        norm_store(sums, 4, 3)
        normed = u_scr[...]
        tile_count = mlp // 256
        ups = [dot(up_w[tile * 256:tile * 256 + 256], normed) for tile in range(tile_count)]

        def gelu(pre):
            return (pre * jnp.tanh(pre * (2.0 * GELU_A + 8.0 * GELU_B * (pre * pre))) + pre).astype(bf16)

        down = [None, None]
        for tile in range(tile_count):
            act = jnp.concatenate([gelu(ups[tile][lo:lo + UNIT]) for lo in range(0, 256, UNIT)], axis=0)
            for side in range(2):
                piece = dot(down_w[side * quarter:side * quarter + quarter, tile * 256:tile * 256 + 256], act)
                down[side] = piece if down[side] is None else down[side] + piece
        for unit in range(2):
            for part in range(each):
                lo = unit * quarter + part * UNIT
                rows = slice(lo, lo + UNIT)
                for half in halves:
                    yield rows, half, h_scr[rows, half] + lanes[5, rows] * down[unit][part * UNIT:part * UNIT + UNIT, half]

    def send(step, columns):
        for rows, half, hidden in columns:
            sent[step, rows, half] = hidden.astype(bf16)
        hidden_copy(step).start()

    def received(step):
        return lambda half, rows=slice(None): recv[step, rows, half].astype(f32)

    def wait_hidden(step):
        @pl.when(step >= 2)
        def _():
            hidden_copy(step - 2).wait_recv()

    def first_step(step, carry):
        @pl.when(step >= 1)
        def _():
            latent_copy(step - 1).wait_recv()
        h_last[...] = dot(w_in_t[...], x_recv[step].astype(bf16))
        send(step, block(step, lambda half, rows=slice(None): h_last[rows, half]))
        return carry

    def middle_step(step, carry):
        wait_hidden(step)
        send(step, block(step, received(step)))
        return carry

    def advance(step):
        normed = jnp.concatenate([normalize(h_last[:, half]).astype(bf16) for half in halves], axis=1)
        noise = dot(w_out_ref[...], normed)
        x_next = keep_ref[step] * x_cur[...] + noise_ref[step] * noise
        x_cur[...] = x_next
        return x_next

    def last_step(sends, step, carry):
        wait_hidden(step)
        before = jnp.maximum(step - 1, 0)

        def beside():
            x_next = jnp.where(step > 0, advance(before), x_ref[...])
            x_cur[...] = x_next
            if sends:
                x_recv[step + 1] = x_next

        def post():
            if sends:
                latent_copy(step).start()

        for rows, half, hidden in block(step, received(step), beside, post):
            h_last[rows, half] = hidden
        return carry

    def final_copy(ahead):
        return pltpu.make_async_remote_copy(
            src_ref=x_cur, dst_ref=out_ref, send_sem=last_send_sem.at[ahead], recv_sem=last_recv_sem,
            device_id={'stage': lax.rem(stage + ahead, stages)}, device_id_type=MESH)

    @pl.when(is_first)
    def _():
        lax.fori_loop(0, first_trips, first_step, 0)

    @pl.when(jnp.logical_not(is_first | is_last))
    def _():
        lax.fori_loop(0, trips, middle_step, 0)

    @pl.when(is_last)
    def _():
        h_last[...] = jnp.zeros_like(h_last)
        lax.fori_loop(0, first_trips - 1, functools.partial(last_step, True), 0)
        lax.fori_loop(first_trips - 1, steps, functools.partial(last_step, False), 0)
        out_ref[...] = advance(steps - 1)
        for ahead in sorted(range(1, stages), key=lambda ahead: -min(ahead, stages - ahead)):
            final_copy(ahead).start()
        for ahead in range(1, stages):
            final_copy(ahead).wait_send()

        def drain(step, carry):
            latent_copy(step).wait_send()
            return carry
        lax.fori_loop(0, first_trips - 1, drain, 0)

    @pl.when(jnp.logical_not(is_last))
    def _():
        def drain(step, carry):
            hidden_copy(step).wait_send()
            return carry
        lax.fori_loop(0, trips, drain, 0)
        final_copy(1).wait_recv()


def solution(mesh):
    stages = mesh.shape['stage']

    def shard_body(x_init, w_in, w_out, w_qkv, w_proj, w_up, w_down, mod_table, coef_keep, coef_noise, h_warm):
        steps = coef_keep.shape[0]
        tokens, chan = x_init.shape[1], x_init.shape[2]
        width, mlp = w_up.shape[1], w_up.shape[2]
        heads, head_dim = w_proj.shape[1], w_proj.shape[2]
        mod_rows = mod_table.shape[2] * width // 128
        bf16, f32 = jnp.bfloat16, jnp.float32
        vmem = pl.BlockSpec(memory_space=pltpu.VMEM)
        smem = pl.BlockSpec(memory_space=pltpu.SMEM)
        hbm = pl.BlockSpec(memory_space=pl.ANY)
        out = pl.pallas_call(
            functools.partial(kernel, stages),
            out_shape=jax.ShapeDtypeStruct((chan, tokens), f32),
            in_specs=[hbm] * 8 + [smem, smem, hbm],
            out_specs=vmem,
            scratch_shapes=[
                pltpu.VMEM((chan, tokens), f32),
                pltpu.VMEM((chan, width), bf16),
                pltpu.VMEM((chan, width), bf16),
                pltpu.VMEM((steps * mod_rows, 128), f32),
                pltpu.VMEM((width, 3 * width), bf16),
                pltpu.VMEM((heads, head_dim, width), bf16),
                pltpu.VMEM((width, mlp), bf16),
                pltpu.VMEM((mlp, width), bf16),
                pltpu.VMEM((2, tokens, width), bf16),
                pltpu.VMEM((width, chan), bf16),
                pltpu.VMEM((3 * width, width), bf16),
                pltpu.VMEM((width, width), bf16),
                pltpu.VMEM((mlp, width), bf16),
                pltpu.VMEM((width, mlp), bf16),
                pltpu.VMEM((steps, 128, 128), bf16),
                pltpu.VMEM((3 * width // 128, 128, 256), bf16),
                pltpu.VMEM((6, width, 128), f32),
                pltpu.VMEM((steps, width, tokens), bf16),
                pltpu.VMEM((steps, width, tokens), bf16),
                pltpu.VMEM((steps, chan, tokens), f32),
                pltpu.VMEM((chan, tokens), f32),
                pltpu.VMEM((width, tokens), f32),
                pltpu.VMEM((width, tokens), f32),
                pltpu.VMEM((width, tokens), bf16),
                pltpu.VMEM((width, tokens), bf16),
                pltpu.VMEM((width, tokens), f32),
                pltpu.SemaphoreType.DMA((9,)),
                pltpu.SemaphoreType.DMA((steps,)),
                pltpu.SemaphoreType.DMA((steps,)),
                pltpu.SemaphoreType.DMA((steps,)),
                pltpu.SemaphoreType.DMA((steps,)),
                pltpu.SemaphoreType.DMA((stages,)),
                pltpu.SemaphoreType.DMA,
            ],
            compiler_params=pltpu.CompilerParams(collective_id=0, has_side_effects=True, vmem_limit_bytes=56 * 1024 * 1024),
            name='stage_loop',
        )(jnp.swapaxes(x_init, 1, 2)[0], w_in, jnp.swapaxes(w_out, 0, 1), w_qkv[0], w_proj[0], w_up[0], w_down[0],
          mod_table.reshape(steps * mod_rows, 128), coef_keep, coef_noise, h_warm)
        return jnp.swapaxes(out, 0, 1)[None]

    return jax.shard_map(
        shard_body,
        mesh=mesh,
        in_specs=(P('data'), P(), P(), P('stage'), P('stage'), P('stage'), P('stage'), P(None, 'stage'), P(), P(), P(None, None, 'data')),
        out_specs=P('data'),
        check_vma=False,
    )
```
